128 devices in a mesh: res: 32 (over x_lo, y, z), seq: 4 (over x_hi, core).
Axes of the slice: x: 4 (x_hi: 2, x_lo: 2; x = x_hi * 2 + x_lo), y: 4, z: 4, core: 2. Of those that a mesh axis runs over, the one named last changes fastest.
Arguments:
- alignment: bfloat16 [384, 1024, 256], P('seq', 'res'), may hold values from -6 to 6
- query_weight: bfloat16 [256, 256], replicated, may hold values from -1 to 1
- w_keyval: bfloat16 [256, 512], replicated, may hold values from -0.375 to 0.375
- w_gate: bfloat16 [256, 256], replicated, may hold values from -0.375 to 0.375
- output_weight: bfloat16 [256, 256], replicated, may hold values from -0.75 to 0.75
- w_factors: bfloat16 [256, 64], replicated, may hold values from -1.5 to 1.5
- w_pair_out: bfloat16 [1024, 128], replicated, may hold values from -0.1875 to 0.1875
Outputs:
- alignment_update: bfloat16 [384, 1024, 256], P('seq', 'res')
- pair_representation_update: bfloat16 [1024, 1024, 128], P(('res', 'seq'))
The draws below stay inside these ranges and needn't reach their ends.
All inputs are finite; a program needn't handle non-finite values.
Results may differ from the reference program's by a relative error of at most 0.012.
The reference program's roundings to bfloat16 on the way count: a program that leaves them out, or rounds other values in their place, can miss the bound.
Values may be sent and summed in bfloat16 or wider, within the bound.
A program may use at most 256 MiB of HBM per device.

```python
import math
import jax
import jax.numpy as jnp
from jax import lax

D = 256
P_SIZE = 128
HEADS = 8
HC = 32
C = 32
HD = 256
S = 384
R = 1024


def levels(own_key, dims, pieces, low, largest):
    gain, own = 1.0, jax.random.fold_in(own_key, 6)
    for position, shards_of in pieces:
        draws = jnp.exp(jax.random.uniform(jax.random.fold_in(own, position), (shards_of,), jnp.float32, low / len(pieces), largest / len(pieces)))
        gain = gain * jnp.repeat(draws, dims[position] // shards_of).reshape([-1 if axis == position else 1 for axis in range(len(dims))])
    return gain


def bell_draw(rng, shape, deviation, bound, pieces=(), held_as=jnp.bfloat16):
    drawn = deviation * jax.random.normal(rng, shape, jnp.float32)
    if pieces:
        drawn = drawn * levels(rng, shape, pieces, -0.22, 0.18)
    return jnp.clip(drawn, -bound, bound).astype(held_as)


def setup_inputs(seed: int = 0) -> dict:
    key_list = jax.random.split(jax.random.key(seed), 8)
    return {
        "alignment": bell_draw(key_list[0], (S, R, D), 1.0, 6.0, ((0, 4), (1, 32))),
        "query_weight": bell_draw(key_list[1], (D, HD), (D // 9) ** -0.5, 1.0),
        "w_keyval": bell_draw(key_list[2], (D, 2 * HD), D ** -0.5, 0.375),
        "w_gate": bell_draw(key_list[3], (D, HD), D ** -0.5, 0.375),
        "output_weight": bell_draw(key_list[4], (HD, D), (HD // 4) ** -0.5, 0.75),
        "w_factors": bell_draw(key_list[5], (D, 2 * C), (D // 16) ** -0.5, 1.5),
        "w_pair_out": bell_draw(key_list[6], (C * C, P_SIZE), (C * C) ** -0.5, 0.1875),
    }


def normalize(alignment):
    values = alignment.astype(jnp.float32)
    centered = values - lax.optimization_barrier(jnp.mean(values, axis=-1, keepdims=True))
    spread = lax.optimization_barrier(jnp.mean(centered * centered, axis=-1, keepdims=True))
    return (centered * lax.rsqrt(spread + 1e-05)).astype(jnp.bfloat16)

def reference(alignment, query_weight, w_keyval, w_gate, output_weight, w_factors, w_pair_out):
    normed = normalize(alignment)
    queries = jnp.dot(normed, query_weight, preferred_element_type=jnp.float32).astype(jnp.bfloat16)
    keyvals = jnp.dot(normed, w_keyval, preferred_element_type=jnp.float32).astype(jnp.bfloat16)
    gating = jax.nn.sigmoid(jnp.dot(normed, w_gate, preferred_element_type=jnp.float32))
    hidden = HEADS * HC
    seq_total = normed.shape[0]
    residues = normed.shape[1]
    group_size = math.gcd(residues, 8)

    def attend_block(block_index):
        start_row = (block_index * group_size).astype(jnp.int32)
        query_block = lax.dynamic_slice_in_dim(queries, start_row, group_size, 1).astype(jnp.float32)
        keyval_block = lax.dynamic_slice_in_dim(keyvals, start_row, group_size, 1).astype(jnp.float32)
        per_head_query = query_block.reshape(seq_total, group_size, HEADS, HC)
        head_keys = keyval_block[:, :, :hidden].reshape(seq_total, group_size, HEADS, HC)
        head_values = keyval_block[:, :, hidden:].reshape(seq_total, group_size, HEADS, HC)
        scores = jnp.einsum('qrhd,krhd->rhqk', per_head_query, head_keys) / math.sqrt(HC)
        exponent = jnp.exp(scores)
        weights = exponent.astype(jnp.bfloat16).astype(jnp.float32)
        denominators = jnp.transpose(lax.optimization_barrier(jnp.sum(exponent, axis=-1)), (2, 0, 1))
        weighted = jnp.einsum('rhqk,krhd->qrhd', weights, head_values)
        return (weighted / denominators[:, :, :, None]).reshape(seq_total, group_size, hidden)
    blocks = lax.map(attend_block, jnp.arange(residues // group_size, dtype=jnp.int32))
    attended = jnp.transpose(blocks, (1, 0, 2, 3)).reshape(seq_total, residues, hidden)
    gated_output_rows = (gating * attended).astype(jnp.bfloat16)
    alignment_update = jnp.dot(gated_output_rows, output_weight, preferred_element_type=jnp.float32).astype(jnp.bfloat16)
    factors = jnp.dot(normed, w_factors, preferred_element_type=jnp.float32).astype(jnp.bfloat16)
    factor = factors.shape[2] // 2
    left_factor = factors[:, :, :factor].astype(jnp.float32).reshape(seq_total, residues * factor)
    right_factor = factors[:, :, factor:].astype(jnp.float32).reshape(seq_total, residues * factor)
    channels = w_pair_out.shape[1]
    pair_weight = w_pair_out.astype(jnp.float32).reshape(factor, factor, channels)
    row_block = math.gcd(residues, 32)

    def pair_block(block_index):
        start_col = (block_index * row_block * factor).astype(jnp.int32)
        left_rows = lax.dynamic_slice_in_dim(left_factor, start_col, row_block * factor, 1)
        products = lax.dot_general(left_rows, right_factor, (((0,), (0,)), ((), ())), precision=lax.Precision.HIGHEST, preferred_element_type=jnp.float32)
        products = (products * (1.0 / seq_total)).reshape(row_block, factor, residues, factor)
        return jnp.einsum('icje,cep->ijp', products, pair_weight, precision=lax.Precision.HIGHEST)
    pair_blocks = lax.map(pair_block, jnp.arange(residues // row_block, dtype=jnp.int32))
    pair_representation_update = pair_blocks.reshape(residues, residues, channels).astype(jnp.bfloat16)
    return (alignment_update, pair_representation_update)
```

```python
import functools
import itertools
import math

import jax
import jax.numpy as jnp
from jax import lax
from jax.experimental import pallas as pl
from jax.experimental.pallas import tpu as pltpu
from jax.sharding import Mesh
from jax.sharding import PartitionSpec as P

HEADS = 8
HC = 32
C = 32
AXES = ("x_lo", "y", "z", "x_hi", "core")
SIZES = (2, 4, 4, 2, 2)
RES = ("x_lo", "y", "z")
SEQ = ("x_hi", "core")
epsilon = 1e-05
VMEM_SPEC = pl.BlockSpec(memory_space=pltpu.VMEM)


def moves(sizes, step):
    def flat(place):
        total = 0
        for size, at in zip(sizes, place):
            total = total * size + at
        return total

    return [(flat(p), flat(step(*p))) for p in itertools.product(*map(range, sizes))]


def to_seq(value, hi, core):
    return lax.ppermute(value, SEQ, moves((2, 2), lambda h, c: (h ^ hi, c ^ core)))


def to_x(value, shift):
    def step(lo, hi):
        x = (hi * 2 + lo + shift) % 4
        return x % 2, x // 2

    return lax.ppermute(value, ("x_lo", "x_hi"), moves((2, 2), step))


def to_y(value, shift):
    return lax.ppermute(value, "y", moves((4,), lambda y: ((y + shift) % 4,)))


def to_z(value, shift, core=0):
    return lax.ppermute(
        value, ("z", "core"), moves((4, 2), lambda z, c: ((z + shift) % 4, c ^ core))
    )


def norm_kernel(place_ref, x_ref, wf_ref, *outs):
    normed_refs, factor_refs = outs[:4], outs[4:]
    own = place_ref[0]
    span = 32
    weight = wf_ref[...].astype(jnp.float32)
    none = jnp.zeros_like(weight)
    even = jnp.concatenate([weight, none], axis=1).astype(jnp.bfloat16)
    odd = jnp.concatenate([none, weight], axis=1).astype(jnp.bfloat16)
    for rel in range(4):
        first = pl.multiple_of((own ^ rel) * 8, 8)
        for part in range(96 // span):
            rows = pl.ds(part * span, span)
            x = x_ref[rows, pl.ds(first, 8), :].astype(jnp.float32)
            centered = x - jnp.mean(x, axis=-1, keepdims=True)
            spread = jnp.mean(centered * centered, axis=-1, keepdims=True)
            normed = centered * lax.rsqrt(spread + epsilon)
            normed_refs[rel][:, rows, :] = jnp.swapaxes(normed, 0, 1).astype(jnp.bfloat16)
        for pair in range(4):
            made = jnp.dot(normed_refs[rel][2 * pair], even, preferred_element_type=jnp.float32)
            made += jnp.dot(normed_refs[rel][2 * pair + 1], odd, preferred_element_type=jnp.float32)
            factor_refs[rel][:, pair * 128 : (pair + 1) * 128] = made.astype(jnp.bfloat16)


def norm_call(place, alignment, w_factors):
    return pl.pallas_call(
        norm_kernel,
        in_specs=[pl.BlockSpec(memory_space=pltpu.SMEM), VMEM_SPEC, VMEM_SPEC],
        out_specs=[VMEM_SPEC] * 8,
        out_shape=[jax.ShapeDtypeStruct((8, 96, 256), jnp.bfloat16)] * 4
        + [jax.ShapeDtypeStruct((96, 512), jnp.bfloat16)] * 4,
        cost_estimate=pl.CostEstimate(flops=2 * 10**9, bytes_accessed=4 * 10**6, transcendentals=0),
        name="norm",
    )(place, alignment, w_factors)


def split_kernel(place_ref, f0, f1, f2, f3, left_ref, right_ref, held):
    own = place_ref[0]
    for rel, ref in enumerate((f0, f1, f2, f3)):
        held[own ^ rel] = ref[...]
    whole = held[...].astype(jnp.float32).reshape(384, 512)
    turned = whole.T.reshape(8, 64, 384)
    left_ref[...] = turned[:, :C].reshape(8 * C, 384).astype(jnp.bfloat16)
    right_ref[...] = jnp.swapaxes(turned[:, C:], 0, 1).astype(jnp.bfloat16)


def split_call(place, parts):
    return pl.pallas_call(
        split_kernel,
        in_specs=[pl.BlockSpec(memory_space=pltpu.SMEM)] + [VMEM_SPEC] * 4,
        out_specs=[VMEM_SPEC] * 2,
        out_shape=[
            jax.ShapeDtypeStruct((8 * C, 384), jnp.bfloat16),
            jax.ShapeDtypeStruct((C, 8, 384), jnp.bfloat16),
        ],
        scratch_shapes=[pltpu.VMEM((4, 96, 512), jnp.bfloat16)],
        cost_estimate=pl.CostEstimate(flops=10**9, bytes_accessed=10**6, transcendentals=0),
        name="split",
    )(place, *parts)


NT = (((1,), (1,)), ((), ()))
TN = (((0,), (0,)), ((), ()))


def attend_kernel(x0, x1, x2, x3, wk_ref, wt_ref, wo_ref, u0, u1, u2, u3, spread_q):
    spread_q[...] = jnp.zeros_like(spread_q)
    ones = jnp.ones((16, 384), jnp.bfloat16)
    scale = 1.0 / math.sqrt(HC)

    def residue(r, _):
        rows = jnp.concatenate([x0[r], x1[r], x2[r], x3[r]], axis=0)
        keys = jnp.dot(rows, wk_ref[...], preferred_element_type=jnp.float32).astype(jnp.bfloat16)
        queries = lax.dot_general(
            wt_ref[:256], rows, NT, preferred_element_type=jnp.float32
        ).astype(jnp.bfloat16)
        values = lax.dot_general(
            wt_ref[256:512], rows, NT, preferred_element_type=jnp.float32
        ).astype(jnp.bfloat16)
        gating = jax.nn.sigmoid(
            lax.dot_general(wt_ref[512:], rows, NT, preferred_element_type=jnp.float32)
        )
        for h in range(HEADS):
            at = slice(h * HC, (h + 1) * HC)
            spread_q[h // 2, at, (h % 2) * 384 : (h % 2 + 1) * 384] = queries[at]
        gated = []
        for pair in range(HEADS // 2):
            scores = jnp.dot(keys, spread_q[pair], preferred_element_type=jnp.float32)
            weights = jnp.exp(scores * scale).astype(jnp.bfloat16)
            for k in range(2):
                h = 2 * pair + k
                at = slice(h * HC, (h + 1) * HC)
                summed = jnp.dot(
                    jnp.concatenate([values[at], ones], axis=0),
                    weights[:, k * 384 : (k + 1) * 384],
                    preferred_element_type=jnp.float32,
                )
                attended = summed[:HC] / summed[HC : HC + 1]
                gated.append((gating[at] * attended).astype(jnp.bfloat16))
        gated = jnp.concatenate(gated, axis=0)
        update = lax.dot_general(
            gated, wo_ref[...], TN, preferred_element_type=jnp.float32
        ).astype(jnp.bfloat16)
        for k, ref in enumerate((u0, u1, u2, u3)):
            ref[r] = update[k * 96 : (k + 1) * 96]
        return 0

    lax.fori_loop(0, 8, residue, 0)


def attend_call(parts, w_key, w_turned, output_weight):
    return pl.pallas_call(
        attend_kernel,
        in_specs=[VMEM_SPEC] * 7,
        out_specs=[VMEM_SPEC] * 4,
        out_shape=[jax.ShapeDtypeStruct((8, 96, 256), jnp.bfloat16)] * 4,
        scratch_shapes=[pltpu.VMEM((4, 256, 768), jnp.bfloat16)],
        cost_estimate=pl.CostEstimate(
            flops=20 * 10**9, bytes_accessed=4 * 10**6, transcendentals=9 * 10**6
        ),
        compiler_params=pltpu.CompilerParams(vmem_limit_bytes=48 * 2**20),
        name="attend",
    )(*parts, w_key, w_turned, output_weight)


def outer_kernel(la, lb, r0, r1, r2, r3, wp_ref, oa, ob, held):
    step = pl.program_id(0)
    left = jnp.concatenate([la[...], lb[...]], axis=0)
    for k in range(4):
        right = jnp.concatenate(
            [ref[2 * k + e] for e in range(2) for ref in (r0, r1, r2, r3)], axis=0
        )
        products = lax.dot_general(left, right, NT, preferred_element_type=jnp.float32).astype(
            jnp.bfloat16
        )
        for e in range(2):
            at = pl.multiple_of((step * 8 + 2 * k + e) * C, C)
            held[:, pl.ds(at, C), :] = products[:, e * 128 : (e + 1) * 128].reshape(16, C, 128)

    @pl.when(step == 3)
    def _():
        for pair in range(8):
            cols = jnp.concatenate([held[2 * pair], held[2 * pair + 1]], axis=1)
            made = jnp.dot(wp_ref[...], cols, preferred_element_type=jnp.float32) * (1.0 / 384)
            for k in range(2):
                i = 2 * pair + k
                block = made[:, k * 128 : (k + 1) * 128].T.astype(jnp.bfloat16)
                (oa if i < 8 else ob)[i % 8] = block


def outer_call(left_a, left_b, rights, w_pair):
    whole = lambda g: (0, 0)
    return pl.pallas_call(
        outer_kernel,
        grid=(4,),
        in_specs=[pl.BlockSpec((256, 384), whole)] * 2
        + [pl.BlockSpec((8, 32, 384), lambda g: (g, 0, 0))] * 4
        + [pl.BlockSpec((128, 1024), whole)],
        out_specs=[pl.BlockSpec((8, 128, 128), lambda g: (0, 0, 0))] * 2,
        out_shape=[jax.ShapeDtypeStruct((8, 128, 128), jnp.bfloat16)] * 2,
        scratch_shapes=[pltpu.VMEM((16, 1024, 128), jnp.bfloat16)],
        cost_estimate=pl.CostEstimate(
            flops=4 * 10**9, bytes_accessed=4 * 10**6, transcendentals=0
        ),
        compiler_params=pltpu.CompilerParams(vmem_limit_bytes=32 * 2**20),
        name="outer",
    )(left_a, left_b, *rights, w_pair)


def place_update_kernel(place_ref, u0, u1, u2, u3, out_ref, turned, sems):
    own = place_ref[0]
    copies = []
    for rel, ref in enumerate((u0, u1, u2, u3)):
        turned[rel] = jnp.swapaxes(ref[...].astype(jnp.float32), 0, 1).astype(jnp.bfloat16)
        first = pl.multiple_of((own ^ rel) * 8, 8)
        copy = pltpu.make_async_copy(
            turned.at[rel], out_ref.at[:, pl.ds(first, 8), :], sems.at[rel]
        )
        copy.start()
        copies.append(copy)
    for copy in copies:
        copy.wait()


def place_update(place, parts):
    return pl.pallas_call(
        place_update_kernel,
        in_specs=[pl.BlockSpec(memory_space=pltpu.SMEM)] + [VMEM_SPEC] * 4,
        out_specs=pl.BlockSpec(memory_space=pl.ANY),
        out_shape=jax.ShapeDtypeStruct((96, 32, 256), jnp.bfloat16),
        scratch_shapes=[
            pltpu.VMEM((4, 96, 8, 256), jnp.bfloat16),
            pltpu.SemaphoreType.DMA((4,)),
        ],
        cost_estimate=pl.CostEstimate(
            flops=2 * 10**9, bytes_accessed=4 * 10**6, transcendentals=0
        ),
        name="place_update",
    )(place, *parts)


def place_pair_kernel(place_ref, *refs):
    parts, out_ref, sem = refs[:8], refs[8], refs[9]
    x, y, z, core = place_ref[1], place_ref[2], place_ref[3], place_ref[4]
    copies = []
    for n, ref in enumerate(parts):
        there_z, there_core = lax.rem(z + n // 2, 4), core ^ (n % 2)
        for dy in range(4):
            there_y = lax.rem(y + dy, 4)
            for dx in range(4):
                there_x = lax.rem(x + dx, 4)
                copy = pltpu.make_async_copy(
                    ref.at[:, dy * 4 + dx],
                    out_ref.at[
                        :, lax.rem(there_x, 2), there_y, there_z, there_x // 2, there_core
                    ],
                    sem,
                )
                copy.start()
                copies.append(copy)
    for copy in copies:
        copy.wait()


def place_pair(place, parts):
    made = pl.pallas_call(
        place_pair_kernel,
        in_specs=[pl.BlockSpec(memory_space=pltpu.SMEM)] + [VMEM_SPEC] * 8,
        out_specs=pl.BlockSpec(memory_space=pl.ANY),
        out_shape=jax.ShapeDtypeStruct((8, 2, 4, 4, 2, 2, 8, 128), jnp.bfloat16),
        scratch_shapes=[pltpu.SemaphoreType.DMA],
        cost_estimate=pl.CostEstimate(
            flops=2 * 10**9, bytes_accessed=4 * 10**6, transcendentals=0
        ),
        name="place_pair",
    )(place, *[p.reshape(8, 16, 8, 128) for p in parts])
    return made.reshape(8, 1024, 128)


def per_device(alignment, query_weight, w_keyval, w_gate, output_weight, w_factors, w_pair_out):
    hi, core = lax.axis_index("x_hi"), lax.axis_index("core")
    place = jnp.stack(
        [
            hi * 2 + core,
            hi * 2 + lax.axis_index("x_lo"),
            lax.axis_index("y"),
            lax.axis_index("z"),
            core,
        ]
    ).astype(jnp.int32)
    w_key = w_keyval[:, :256]
    w_turned = jnp.concatenate([query_weight, w_keyval[:, 256:], w_gate], axis=1).T
    w_pair = w_pair_out.reshape(C, C, 128).transpose(2, 1, 0).reshape(128, C * C)

    made = norm_call(place, alignment, w_factors)
    normed, factors = made[:4], made[4:]
    rels = [(0, 1), (1, 0), (1, 1)]
    factors = [factors[0]] + [to_seq(factors[n + 1], *rel) for n, rel in enumerate(rels)]
    normed = [normed[0]] + [to_seq(normed[n + 1], *rel) for n, rel in enumerate(rels)]
    left, right = split_call(place, factors)

    right_x = jnp.concatenate([right] + [to_x(right, -dx) for dx in (1, 2, 3)], axis=1)
    rights = [right_x] + [to_y(right_x, -dy) for dy in (1, 2, 3)]
    lefts = jnp.stack([left] + [to_z(left, -dz) for dz in (1, 2, 3)])
    lefts_other = to_z(lefts, 0, 1)

    update = attend_call(normed, w_key, w_turned, output_weight)
    update = [update[0]] + [to_seq(update[n + 1], *rel) for n, rel in enumerate(rels)]

    pieces = [None] * 8
    for dz in (2, 1, 3, 0):
        same, other = outer_call(lefts[dz], lefts_other[dz], rights, w_pair)
        back = (4 - dz) % 4
        pieces[2 * back] = to_z(same, dz) if dz else same
        pieces[2 * back + 1] = to_z(other, dz, 1)
    alignment_update = place_update(place, update)
    pair_update = place_pair(place, pieces)
    return (alignment_update, pair_update)


def solution(mesh):
    split = Mesh(mesh.devices.reshape(SIZES), AXES)
    in_specs = (P(SEQ, RES, None), P(), P(), P(), P(), P(), P())
    out_specs = (P(SEQ, RES, None), P(AXES, None, None))
    return jax.shard_map(
        per_device, mesh=split, in_specs=in_specs, out_specs=out_specs, check_vma=False
    )
```

```python
import math

import jax
import jax.numpy as jnp
from jax import lax
from jax.experimental import pallas as pl
from jax.experimental.pallas import tpu as pltpu
from jax.sharding import Mesh
from jax.sharding import PartitionSpec as P

HEADS = 8
HC = 32
C = 32
AXES = ("x_lo", "y", "z", "x_hi", "core")
SIZES = (2, 4, 4, 2, 2)
RES = ("x_lo", "y", "z")
SEQ = ("x_hi", "core")
epsilon = 1e-05
NT = (((1,), (1,)), ((), ()))
TN = (((0,), (0,)), ((), ()))
RELS = ((0, 0), (0, 1), (1, 0), (1, 1))
CHUNKS = 4
PER_CHUNK = 8 // CHUNKS
F32 = jnp.float32
BF16 = jnp.bfloat16
VMEM_SPEC = pl.BlockSpec(memory_space=pltpu.VMEM)
ANY_SPEC = pl.BlockSpec(memory_space=pl.ANY)
MESH = pl.DeviceIdType.MESH


def flipped(value, flip):
    return 1 - value if flip else value


def seq_of(rel):
    hi, core = lax.axis_index("x_hi"), lax.axis_index("core")
    return flipped(hi, RELS[rel][0]) * 2 + flipped(core, RELS[rel][1])


def seq_device(rel):
    hi, core = lax.axis_index("x_hi"), lax.axis_index("core")
    return {"x_hi": flipped(hi, RELS[rel][0]), "core": flipped(core, RELS[rel][1])}


def x_device(shift):
    x = lax.axis_index("x_hi") * 2 + lax.axis_index("x_lo")
    there = lax.rem(x + shift + 4, 4)
    return {"x_lo": lax.rem(there, 2), "x_hi": there // 2}


def y_device(shift):
    return {"y": lax.rem(lax.axis_index("y") + shift + 4, 4)}


def z_device(shift, flip):
    there = lax.rem(lax.axis_index("z") + shift + 4, 4)
    return {"z": there, "core": flipped(lax.axis_index("core"), flip)}


def remote(src, dst, send, recv, device):
    return pltpu.make_async_remote_copy(
        src_ref=src, dst_ref=dst, send_sem=send, recv_sem=recv, device_id=device, device_id_type=MESH
    )


def step_kernel(
    x_ref, wf_ref, wq_ref, wkv_ref, wg_ref, wo_ref, wp_ref,
    update_out, pair_out,
    normed_out, rows_in, factors_out, factors_in, rights, lefts, spread_q, w_turned, w_pair,
    update_made, aligned, held, blocks,
    f_send, f_recv, n_send, n_recv, x_send, x_recv, y_send, y_recv, w_send, w_recv,
    l_send, l_recv, u_send, u_recv, p_send, p_recv, own_sem,
):
    barrier = pltpu.get_barrier_semaphore()
    partners = [seq_device(rel) for rel in (1, 2, 3)] + [x_device(1), x_device(-1)]
    partners += [y_device(1), y_device(-1)]
    partners += [z_device(dz, dc) for dz in (1, 2, 3) for dc in (0, 1)]
    for device in partners:
        pl.semaphore_signal(barrier, inc=1, device_id=device, device_id_type=MESH)

    def factor_copy(rel):
        return remote(
            factors_out.at[rel - 1], factors_in.at[seq_of(0)],
            f_send.at[rel - 1], f_recv.at[rel - 1], seq_device(rel),
        )

    def normed_copy(rel, chunk):
        part = pl.ds(chunk * PER_CHUNK, PER_CHUNK)
        return remote(
            normed_out.at[rel - 1, part], rows_in.at[rel, part],
            n_send.at[rel - 1, chunk], n_recv.at[rel - 1, chunk], seq_device(rel),
        )

    def x_copy(dx):
        return remote(
            rights.at[0, 0], rights.at[0, dx], x_send.at[dx - 1], x_recv.at[dx - 1], x_device(-dx)
        )

    def y_copy(dx, way):
        return remote(
            rights.at[0, dx], rights.at[(1, 3)[way], dx],
            y_send.at[dx, way], y_recv.at[dx, way], y_device((-1, 1)[way]),
        )

    def relay_copy(dx, way):
        half = pl.ds(16 * way, 16)
        return remote(
            rights.at[(1, 3)[way], dx, half], rights.at[2, dx, half],
            w_send.at[dx, way], w_recv.at[dx, way], y_device((-1, 1)[way]),
        )

    def left_copy(n):
        dz, dc = n // 2, n % 2
        return remote(
            lefts.at[0, 0], lefts.at[dz, dc], l_send.at[n - 1], l_recv.at[n - 1], z_device(-dz, dc)
        )

    def update_copy(rel, chunk):
        part = pl.ds(chunk * PER_CHUNK, PER_CHUNK)
        return remote(
            update_made.at[rel, part], update_out.at[rel, part],
            u_send.at[rel - 1, chunk], u_recv.at[rel - 1, chunk], seq_device(rel),
        )

    def block_copy(n):
        dz, dc = n // 2, n % 2
        there = 2 * ((4 - dz) % 4) + dc
        return remote(
            blocks.at[n], pair_out.at[there], p_send.at[n - 1], p_recv.at[there - 1],
            z_device(dz, dc),
        )

    weight = wf_ref[...]
    none = jnp.zeros_like(weight)
    even = jnp.concatenate([weight, none], axis=0)
    odd = jnp.concatenate([none, weight], axis=0)
    span = 32
    for rel in (1, 2, 3, 0):
        first = pl.multiple_of(seq_of(rel) * 8, 8)
        normed_ref = normed_out.at[rel - 1] if rel else rows_in.at[0]
        factor_ref = factors_out.at[rel - 1] if rel else factors_in.at[seq_of(0)]

        def norm_rows(part, _, first=first, normed_ref=normed_ref):
            rows = pl.ds(pl.multiple_of(part * span, span), span)
            x = x_ref[rows, pl.ds(first, 8), :].astype(F32)
            centered = x - jnp.mean(x, axis=-1, keepdims=True)
            spread = jnp.mean(centered * centered, axis=-1, keepdims=True)
            normed = centered * lax.rsqrt(spread + epsilon)
            normed_ref[:, rows, :] = jnp.swapaxes(normed, 0, 1).astype(BF16)
            return 0

        lax.fori_loop(0, 96 // span, norm_rows, 0, unroll=True)
        for pair in range(4):
            made = lax.dot_general(
                normed_ref[2 * pair], even, NT, preferred_element_type=F32
            ) + lax.dot_general(normed_ref[2 * pair + 1], odd, NT, preferred_element_type=F32)
            factor_ref[:, pair * 128 : (pair + 1) * 128] = made.astype(BF16)
        if rel == 1:
            pl.semaphore_wait(barrier, len(partners))
        if rel:
            factor_copy(rel).start()
    for rel in (1, 2, 3):
        normed_copy(rel, 0).start()

    w_turned[:256] = wq_ref[...].astype(F32).T.astype(BF16)
    w_turned[256:512] = wkv_ref[:, 256:].astype(F32).T.astype(BF16)
    w_turned[512:] = wg_ref[...].astype(F32).T.astype(BF16)
    pair_rows = jnp.swapaxes(wp_ref[...].astype(F32).reshape(C, C, 128), 0, 1)
    w_pair[...] = pair_rows.reshape(C * C, 128).T.astype(BF16)
    spread_q[...] = jnp.zeros_like(spread_q)

    for rel in (1, 2, 3):
        factor_copy(rel).wait_recv()
    turned = factors_in[...].astype(F32).reshape(384, 512).T.reshape(8, 64, 384)
    rights[0, 0] = jnp.swapaxes(turned[:, C:], 0, 1).astype(BF16)
    lefts[0, 0] = turned[:, :C].reshape(8 * C, 384).astype(BF16)
    for dx in (1, 3, 2):
        x_copy(dx).start()
    for way in (0, 1):
        y_copy(0, way).start()
    for n in range(1, 8):
        left_copy(n).start()
    for chunk in range(1, CHUNKS):
        for rel in (1, 2, 3):
            normed_copy(rel, chunk).start()

    ones = jnp.ones((16, 384), BF16)
    scale = 1.0 / math.sqrt(HC)

    def residue(r, _):
        rows = jnp.concatenate([rows_in[k, r] for k in range(4)], axis=0)
        keys = jnp.dot(rows, wkv_ref[:, :256], preferred_element_type=F32).astype(BF16)
        queries = lax.dot_general(w_turned[:256], rows, NT, preferred_element_type=F32).astype(BF16)
        values = lax.dot_general(
            w_turned[256:512], rows, NT, preferred_element_type=F32
        ).astype(BF16)
        gating = jax.nn.sigmoid(
            lax.dot_general(w_turned[512:], rows, NT, preferred_element_type=F32)
        )
        for h in range(HEADS):
            at = slice(h * HC, (h + 1) * HC)
            spread_q[h // 2, at, (h % 2) * 384 : (h % 2 + 1) * 384] = queries[at]
        gated = []
        for pair in range(HEADS // 2):
            scores = jnp.dot(keys, spread_q[pair], preferred_element_type=F32)
            weights = jnp.exp(scores * scale).astype(BF16)
            for k in range(2):
                h = 2 * pair + k
                at = slice(h * HC, (h + 1) * HC)
                summed = jnp.dot(
                    jnp.concatenate([values[at], ones], axis=0),
                    weights[:, k * 384 : (k + 1) * 384],
                    preferred_element_type=F32,
                )
                attended = summed[:HC] / summed[HC : HC + 1]
                gated.append((gating[at] * attended).astype(BF16))
        update = lax.dot_general(
            jnp.concatenate(gated, axis=0), wo_ref[...], TN, preferred_element_type=F32
        ).astype(BF16)
        for k in range(4):
            update_made[k, r] = update[k * 96 : (k + 1) * 96]
        return 0

    def chunk_step(chunk, _):
        for rel in (1, 2, 3):
            normed_copy(rel, chunk).wait_recv()
        lax.fori_loop(chunk * PER_CHUNK, (chunk + 1) * PER_CHUNK, residue, 0)
        for rel in (1, 2, 3):
            update_copy(rel, chunk).start()

        @pl.when(chunk == 0)
        def _():
            for dx in (1, 3):
                x_copy(dx).wait_recv()
                for way in (0, 1):
                    y_copy(dx, way).start()
            for way in (0, 1):
                y_copy(0, way).wait_recv()
                relay_copy(0, way).start()
            x_copy(2).wait_recv()
            for way in (0, 1):
                y_copy(2, way).start()

        @pl.when(chunk == 1)
        def _():
            for dx in (1, 3):
                for way in (0, 1):
                    y_copy(dx, way).wait_recv()
                    relay_copy(dx, way).start()

        @pl.when(chunk == 2)
        def _():
            for way in (0, 1):
                y_copy(2, way).wait_recv()
                relay_copy(2, way).start()

        return 0

    lax.fori_loop(0, CHUNKS, chunk_step, 0)

    own_update = pltpu.make_async_copy(update_made.at[0], update_out.at[0], own_sem.at[0])
    own_update.start()

    for dx in range(4):
        for way in (0, 1):
            relay_copy(dx, way).wait_recv()

    def align(e, _):
        aligned[e] = jnp.concatenate(
            [rights[dy, dx, e] for dy in range(4) for dx in range(4)], axis=0
        )
        return 0

    lax.fori_loop(0, C, align, 0)
    for n in range(1, 8):
        left_copy(n).wait_recv()

    for dz in (2, 1, 3, 0):
        left = lefts.at[dz]

        def products(k, _, left=left):
            right = aligned[pl.ds(2 * k, 2)].reshape(256, 384)
            made = lax.dot_general(
                left[...].reshape(512, 384), right, NT, preferred_element_type=F32
            ).astype(BF16)
            for e in range(2):
                at = pl.multiple_of((2 * k + e) * C, C)
                held[:, pl.ds(at, C), :] = made[:, e * 128 : (e + 1) * 128].reshape(16, C, 128)
            return 0

        lax.fori_loop(0, C // 2, products, 0)
        for dc in (0, 1):

            def project(pair, _, dz=dz, dc=dc):
                i = 8 * dc + 2 * pair
                cols = jnp.concatenate([held[i], held[i + 1]], axis=1)
                made = jnp.dot(w_pair[...], cols, preferred_element_type=F32) * (1.0 / 384)
                for k in range(2):
                    blocks[2 * dz + dc, 2 * pair + k] = (
                        made[:, k * 128 : (k + 1) * 128].T.astype(BF16)
                    )
                return 0

            lax.fori_loop(0, 4, project, 0)
            if dz or dc:
                block_copy(2 * dz + dc).start()
    own_block = pltpu.make_async_copy(blocks.at[0], pair_out.at[0], own_sem.at[1])
    own_block.start()

    for rel in (1, 2, 3):
        factor_copy(rel).wait_send()
        for chunk in range(CHUNKS):
            normed_copy(rel, chunk).wait_send()
            update_copy(rel, chunk).wait()
    for dx in (1, 2, 3):
        x_copy(dx).wait_send()
    for dx in range(4):
        for way in (0, 1):
            y_copy(dx, way).wait_send()
            relay_copy(dx, way).wait_send()
    for n in range(1, 8):
        left_copy(n).wait_send()
    own_update.wait()
    own_block.wait()
    for n in range(1, 8):
        block_copy(n).wait()


def step_call(alignment, w_factors, query_weight, w_keyval, w_gate, output_weight, w_pair_out):
    dma = pltpu.SemaphoreType.DMA
    return pl.pallas_call(
        step_kernel,
        in_specs=[VMEM_SPEC] * 7,
        out_specs=[ANY_SPEC] * 2,
        out_shape=[
            jax.ShapeDtypeStruct((4, 8, 96, 256), BF16),
            jax.ShapeDtypeStruct((8, 8, 128, 128), BF16),
        ],
        scratch_shapes=[
            pltpu.VMEM((3, 8, 96, 256), BF16),
            pltpu.VMEM((4, 8, 96, 256), BF16),
            pltpu.VMEM((3, 96, 512), BF16),
            pltpu.VMEM((4, 96, 512), BF16),
            pltpu.VMEM((4, 4, C, 8, 384), BF16),
            pltpu.VMEM((4, 2, 8 * C, 384), BF16),
            pltpu.VMEM((4, 256, 768), BF16),
            pltpu.VMEM((768, 256), BF16),
            pltpu.VMEM((128, C * C), BF16),
            pltpu.VMEM((4, 8, 96, 256), BF16),
            pltpu.VMEM((C, 128, 384), BF16),
            pltpu.VMEM((16, C * C, 128), BF16),
            pltpu.VMEM((8, 8, 128, 128), BF16),
            dma((3,)), dma((3,)), dma((3, CHUNKS)), dma((3, CHUNKS)), dma((3,)), dma((3,)),
            dma((4, 2)), dma((4, 2)), dma((4, 2)), dma((4, 2)), dma((7,)), dma((7,)),
            dma((3, CHUNKS)), dma((3, CHUNKS)), dma((7,)), dma((7,)), dma((2,)),
        ],
        compiler_params=pltpu.CompilerParams(
            collective_id=0, has_side_effects=True, vmem_limit_bytes=58 * 2**20
        ),
        name="step",
    )(alignment, w_factors.T, query_weight, w_keyval, w_gate, output_weight, w_pair_out)


def place_update_kernel(parts, out_ref, turned, sems):
    copies = []
    for rel in range(4):
        turned[rel] = jnp.swapaxes(parts[rel].astype(F32), 0, 1).astype(BF16)
        first = pl.multiple_of(seq_of(rel) * 8, 8)
        copy = pltpu.make_async_copy(
            turned.at[rel], out_ref.at[:, pl.ds(first, 8), :], sems.at[rel]
        )
        copy.start()
        copies.append(copy)
    for copy in copies:
        copy.wait()


def place_update(parts):
    return pl.pallas_call(
        place_update_kernel,
        in_specs=[VMEM_SPEC],
        out_specs=ANY_SPEC,
        out_shape=jax.ShapeDtypeStruct((96, 32, 256), BF16),
        scratch_shapes=[
            pltpu.VMEM((4, 96, 8, 256), BF16),
            pltpu.SemaphoreType.DMA((4,)),
        ],
        name="place_update",
    )(parts)


def place_pair_kernel(parts, out_ref, sem):
    x = lax.axis_index("x_hi") * 2 + lax.axis_index("x_lo")
    y, z, core = lax.axis_index("y"), lax.axis_index("z"), lax.axis_index("core")
    copies = []
    for n in range(8):
        there_z, there_core = lax.rem(z + n // 2, 4), flipped(core, n % 2)
        for dy in range(4):
            there_y = lax.rem(y + dy, 4)
            for dx in range(4):
                there_x = lax.rem(x + dx, 4)
                copy = pltpu.make_async_copy(
                    parts.at[n, :, dy * 4 + dx],
                    out_ref.at[
                        :, lax.rem(there_x, 2), there_y, there_z, there_x // 2, there_core
                    ],
                    sem,
                )
                copy.start()
                copies.append(copy)
    for copy in copies:
        copy.wait()


def place_pair(parts):
    made = pl.pallas_call(
        place_pair_kernel,
        in_specs=[VMEM_SPEC],
        out_specs=ANY_SPEC,
        out_shape=jax.ShapeDtypeStruct((8, 2, 4, 4, 2, 2, 8, 128), BF16),
        scratch_shapes=[pltpu.SemaphoreType.DMA],
        name="place_pair",
    )(parts.reshape(8, 8, 16, 8, 128))
    return made.reshape(8, 1024, 128)


def per_device(alignment, query_weight, w_keyval, w_gate, output_weight, w_factors, w_pair_out):
    update, pieces = step_call(
        alignment, w_factors, query_weight, w_keyval, w_gate, output_weight, w_pair_out
    )
    return (place_update(update), place_pair(pieces))


def solution(mesh):
    split = Mesh(mesh.devices.reshape(SIZES), AXES)
    in_specs = (P(SEQ, RES, None), P(), P(), P(), P(), P(), P())
    out_specs = (P(SEQ, RES, None), P(AXES, None, None))
    return jax.shard_map(
        per_device, mesh=split, in_specs=in_specs, out_specs=out_specs, check_vma=False
    )
```

```python
import math

import jax
import jax.numpy as jnp
from jax import lax
from jax.experimental import pallas as pl
from jax.experimental.pallas import tpu as pltpu
from jax.sharding import Mesh
from jax.sharding import PartitionSpec as P

HEADS = 8
HC = 32
C = 32
AXES = ("x_lo", "y", "z", "x_hi", "core")
SIZES = (2, 4, 4, 2, 2)
RES = ("x_lo", "y", "z")
SEQ = ("x_hi", "core")
epsilon = 1e-05
NT = (((1,), (1,)), ((), ()))
TN = (((0,), (0,)), ((), ()))
RELS = ((0, 0), (0, 1), (1, 0), (1, 1))
CHUNKS = 4
PER_CHUNK = 8 // CHUNKS
F32 = jnp.float32
BF16 = jnp.bfloat16
VMEM_SPEC = pl.BlockSpec(memory_space=pltpu.VMEM)
ANY_SPEC = pl.BlockSpec(memory_space=pl.ANY)
MESH = pl.DeviceIdType.MESH


def flipped(value, flip):
    return 1 - value if flip else value


def seq_of(rel):
    hi, core = lax.axis_index("x_hi"), lax.axis_index("core")
    return flipped(hi, RELS[rel][0]) * 2 + flipped(core, RELS[rel][1])


def seq_device(rel):
    hi, core = lax.axis_index("x_hi"), lax.axis_index("core")
    return {"x_hi": flipped(hi, RELS[rel][0]), "core": flipped(core, RELS[rel][1])}


def x_device(shift):
    x = lax.axis_index("x_hi") * 2 + lax.axis_index("x_lo")
    there = lax.rem(x + shift + 4, 4)
    return {"x_lo": lax.rem(there, 2), "x_hi": there // 2}


def gather_device(shift, flip=0):
    core = lax.axis_index("core")
    return {
        "y": lax.rem(lax.axis_index("y") + (1 - core) * (shift + 4), 4),
        "z": lax.rem(lax.axis_index("z") + core * (shift + 4), 4),
        "core": flipped(core, flip),
    }


def share_device(shift, flip=0):
    core = lax.axis_index("core")
    return {
        "y": lax.rem(lax.axis_index("y") + core * (shift + 4), 4),
        "z": lax.rem(lax.axis_index("z") + (1 - core) * (shift + 4), 4),
        "core": flipped(core, flip),
    }


def remote(src, dst, send, recv, device):
    return pltpu.make_async_remote_copy(
        src_ref=src, dst_ref=dst, send_sem=send, recv_sem=recv, device_id=device, device_id_type=MESH
    )


def step_kernel(
    x_ref, wf_ref, wq_ref, wkv_ref, wg_ref, wo_ref, wp_ref,
    update_out, pair_out,
    normed_out, rows_in, factors_out, factors_in, rights, lefts, spread_q, w_turned, w_pair,
    update_made, aligned, held, blocks,
    f_send, f_recv, n_send, n_recv, x_send, x_recv, y_send, y_recv, w_send, w_recv,
    l_send, l_recv, u_send, u_recv, p_send, p_recv, own_sem,
):
    barrier = pltpu.get_barrier_semaphore()
    partners = [seq_device(rel) for rel in (1, 2, 3)] + [x_device(1), x_device(-1)]
    partners += [gather_device(1), gather_device(-1)]
    partners += [share_device(shift, flip) for shift in (1, 2, 3) for flip in (0, 1)]
    partners += [gather_device(shift, 1) for shift in (1, 2, 3)]
    for device in partners:
        pl.semaphore_signal(barrier, inc=1, device_id=device, device_id_type=MESH)

    def factor_copy(rel):
        return remote(
            factors_out.at[rel - 1], factors_in.at[seq_of(0)],
            f_send.at[rel - 1], f_recv.at[rel - 1], seq_device(rel),
        )

    def normed_copy(rel, chunk):
        part = pl.ds(chunk * PER_CHUNK, PER_CHUNK)
        return remote(
            normed_out.at[rel - 1, part], rows_in.at[rel, part],
            n_send.at[rel - 1, chunk], n_recv.at[rel - 1, chunk], seq_device(rel),
        )

    def x_copy(dx):
        return remote(
            rights.at[0, 0], rights.at[0, dx], x_send.at[dx - 1], x_recv.at[dx - 1], x_device(-dx)
        )

    def y_copy(dx, way):
        return remote(
            rights.at[0, dx], rights.at[(1, 3)[way], dx],
            y_send.at[dx, way], y_recv.at[dx, way], gather_device((-1, 1)[way]),
        )

    def relay_copy(dx, way):
        half = pl.ds(16 * way, 16)
        return remote(
            rights.at[(1, 3)[way], dx, half], rights.at[2, dx, half],
            w_send.at[dx, way], w_recv.at[dx, way], gather_device((-1, 1)[way]),
        )

    def left_copy(n):
        away, flip = n // 2, n % 2
        device = gather_device(-away, 1) if flip else share_device(-away)
        return remote(
            lefts.at[0, 0], lefts.at[away, flip], l_send.at[n - 1], l_recv.at[n - 1], device
        )

    def update_copy(rel, chunk):
        part = pl.ds(chunk * PER_CHUNK, PER_CHUNK)
        return remote(
            update_made.at[rel, part], update_out.at[rel, part],
            u_send.at[rel - 1, chunk], u_recv.at[rel - 1, chunk], seq_device(rel),
        )

    def block_copy(n):
        dz, dc = n // 2, n % 2
        there = 2 * ((4 - dz) % 4) + dc
        return remote(
            blocks.at[n], pair_out.at[there], p_send.at[n - 1], p_recv.at[there - 1],
            share_device(dz, dc),
        )

    weight = wf_ref[...]
    none = jnp.zeros_like(weight)
    even = jnp.concatenate([weight, none], axis=0)
    odd = jnp.concatenate([none, weight], axis=0)
    span = 32
    for rel in (2, 3, 1, 0):
        first = pl.multiple_of(seq_of(rel) * 8, 8)
        normed_ref = normed_out.at[rel - 1] if rel else rows_in.at[0]
        factor_ref = factors_out.at[rel - 1] if rel else factors_in.at[seq_of(0)]

        def norm_rows(part, _, first=first, normed_ref=normed_ref):
            rows = pl.ds(pl.multiple_of(part * span, span), span)
            x = x_ref[rows, pl.ds(first, 8), :].astype(F32)
            centered = x - jnp.mean(x, axis=-1, keepdims=True)
            spread = jnp.mean(centered * centered, axis=-1, keepdims=True)
            normed = centered * lax.rsqrt(spread + epsilon)
            normed_ref[:, rows, :] = jnp.swapaxes(normed, 0, 1).astype(BF16)
            return 0

        lax.fori_loop(0, 96 // span, norm_rows, 0, unroll=True)
        for pair in range(4):
            made = lax.dot_general(
                normed_ref[2 * pair], even, NT, preferred_element_type=F32
            ) + lax.dot_general(normed_ref[2 * pair + 1], odd, NT, preferred_element_type=F32)
            factor_ref[:, pair * 128 : (pair + 1) * 128] = made.astype(BF16)
        if rel == 2:
            pl.semaphore_wait(barrier, len(partners))
        if rel:
            factor_copy(rel).start()
    for rel in (1, 2, 3):
        normed_copy(rel, 0).start()

    w_turned[:256] = wq_ref[...].astype(F32).T.astype(BF16)
    w_turned[256:512] = wkv_ref[:, 256:].astype(F32).T.astype(BF16)
    w_turned[512:] = wg_ref[...].astype(F32).T.astype(BF16)
    pair_rows = jnp.swapaxes(wp_ref[...].astype(F32).reshape(C, C, 128), 0, 1)
    w_pair[...] = pair_rows.reshape(C * C, 128).T.astype(BF16)
    spread_q[...] = jnp.zeros_like(spread_q)

    for rel in (1, 2, 3):
        factor_copy(rel).wait_recv()
    turned = factors_in[...].astype(F32).reshape(384, 512).T.reshape(8, 64, 384)
    rights[0, 0] = jnp.swapaxes(turned[:, C:], 0, 1).astype(BF16)
    lefts[0, 0] = turned[:, :C].reshape(8 * C, 384).astype(BF16)
    for dx in (1, 3, 2):
        x_copy(dx).start()
    for way in (0, 1):
        y_copy(0, way).start()
    for n in range(1, 8):
        left_copy(n).start()
    for chunk in range(1, CHUNKS):
        for rel in (1, 2, 3):
            normed_copy(rel, chunk).start()

    ones = jnp.ones((16, 384), BF16)
    scale = math.log2(math.e) / math.sqrt(HC)

    def residue(r, slot):
        rows = jnp.concatenate([rows_in[k, r] for k in range(4)], axis=0)
        keys = jnp.dot(rows, wkv_ref[:, :256], preferred_element_type=F32).astype(BF16)
        queries = lax.dot_general(w_turned[:256], rows, NT, preferred_element_type=F32).astype(BF16)
        values = lax.dot_general(
            w_turned[256:512], rows, NT, preferred_element_type=F32
        ).astype(BF16)
        gating = jax.nn.sigmoid(
            lax.dot_general(w_turned[512:], rows, NT, preferred_element_type=F32)
        )
        for h in range(HEADS):
            at = slice(h * HC, (h + 1) * HC)
            spread_q[slot, h // 2, at, (h % 2) * 384 : (h % 2 + 1) * 384] = queries[at]
        gated = []
        for pair in range(HEADS // 2):
            scores = jnp.dot(keys, spread_q[slot, pair], preferred_element_type=F32)
            weights = jnp.exp2(scores * scale).astype(BF16)
            for k in range(2):
                h = 2 * pair + k
                at = slice(h * HC, (h + 1) * HC)
                summed = jnp.dot(
                    jnp.concatenate([values[at], ones], axis=0),
                    weights[:, k * 384 : (k + 1) * 384],
                    preferred_element_type=F32,
                )
                attended = summed[:HC] / summed[HC : HC + 1]
                gated.append((gating[at] * attended).astype(BF16))
        update = lax.dot_general(
            jnp.concatenate(gated, axis=0), wo_ref[...], TN, preferred_element_type=F32
        ).astype(BF16)
        for k in range(4):
            update_made[k, r] = update[k * 96 : (k + 1) * 96]

    def chunk_step(chunk, _):
        for rel in (1, 2, 3):
            normed_copy(rel, chunk).wait_recv()
        for k in range(PER_CHUNK):
            residue(chunk * PER_CHUNK + k, k)
        for rel in (1, 2, 3):
            update_copy(rel, chunk).start()

        @pl.when(chunk == 0)
        def _():
            for dx in (1, 3):
                x_copy(dx).wait_recv()
                for way in (0, 1):
                    y_copy(dx, way).start()
            for way in (0, 1):
                y_copy(0, way).wait_recv()
                relay_copy(0, way).start()
            x_copy(2).wait_recv()
            for way in (0, 1):
                y_copy(2, way).start()

        @pl.when(chunk == 1)
        def _():
            for dx in (1, 3):
                for way in (0, 1):
                    y_copy(dx, way).wait_recv()
                    relay_copy(dx, way).start()

        @pl.when(chunk == 2)
        def _():
            for way in (0, 1):
                y_copy(2, way).wait_recv()
                relay_copy(2, way).start()

        return 0

    lax.fori_loop(0, CHUNKS, chunk_step, 0)

    own_update = pltpu.make_async_copy(update_made.at[0], update_out.at[0], own_sem.at[0])
    own_update.start()

    for dx in range(4):
        for way in (0, 1):
            relay_copy(dx, way).wait_recv()

    def align(e, _):
        aligned[e] = jnp.concatenate(
            [rights[dy, dx, e] for dy in range(4) for dx in range(4)], axis=0
        )
        return 0

    lax.fori_loop(0, C, align, 0, unroll=4)
    for n in range(1, 8):
        left_copy(n).wait_recv()

    for dz in (2, 1, 3, 0):
        left = lefts.at[dz]

        def products(k, _, left=left):
            right = aligned[pl.ds(2 * k, 2)].reshape(256, 384)
            made = lax.dot_general(
                left[...].reshape(512, 384), right, NT, preferred_element_type=F32
            ).astype(BF16)
            for e in range(2):
                at = pl.multiple_of((2 * k + e) * C, C)
                held[:, pl.ds(at, C), :] = made[:, e * 128 : (e + 1) * 128].reshape(16, C, 128)
            return 0

        lax.fori_loop(0, C // 2, products, 0, unroll=4)
        for dc in (0, 1):

            def project(pair, _, dz=dz, dc=dc):
                i = 8 * dc + 2 * pair
                cols = jnp.concatenate([held[i], held[i + 1]], axis=1)
                made = jnp.dot(w_pair[...], cols, preferred_element_type=F32) * (1.0 / 384)
                for k in range(2):
                    blocks[2 * dz + dc, 2 * pair + k] = (
                        made[:, k * 128 : (k + 1) * 128].T.astype(BF16)
                    )
                return 0

            lax.fori_loop(0, 4, project, 0, unroll=True)
            if dz or dc:
                block_copy(2 * dz + dc).start()
    own_block = pltpu.make_async_copy(blocks.at[0], pair_out.at[0], own_sem.at[1])
    own_block.start()

    for rel in (1, 2, 3):
        factor_copy(rel).wait_send()
        for chunk in range(CHUNKS):
            normed_copy(rel, chunk).wait_send()
            update_copy(rel, chunk).wait()
    for dx in (1, 2, 3):
        x_copy(dx).wait_send()
    for dx in range(4):
        for way in (0, 1):
            y_copy(dx, way).wait_send()
            relay_copy(dx, way).wait_send()
    for n in range(1, 8):
        left_copy(n).wait_send()
    own_update.wait()
    own_block.wait()
    for n in range(1, 8):
        block_copy(n).wait()


def step_call(alignment, w_factors, query_weight, w_keyval, w_gate, output_weight, w_pair_out):
    dma = pltpu.SemaphoreType.DMA
    return pl.pallas_call(
        step_kernel,
        in_specs=[VMEM_SPEC] * 7,
        out_specs=[ANY_SPEC] * 2,
        out_shape=[
            jax.ShapeDtypeStruct((4, 8, 96, 256), BF16),
            jax.ShapeDtypeStruct((8, 8, 128, 128), BF16),
        ],
        scratch_shapes=[
            pltpu.VMEM((3, 8, 96, 256), BF16),
            pltpu.VMEM((4, 8, 96, 256), BF16),
            pltpu.VMEM((3, 96, 512), BF16),
            pltpu.VMEM((4, 96, 512), BF16),
            pltpu.VMEM((4, 4, C, 8, 384), BF16),
            pltpu.VMEM((4, 2, 8 * C, 384), BF16),
            pltpu.VMEM((PER_CHUNK, 4, 256, 768), BF16),
            pltpu.VMEM((768, 256), BF16),
            pltpu.VMEM((128, C * C), BF16),
            pltpu.VMEM((4, 8, 96, 256), BF16),
            pltpu.VMEM((C, 128, 384), BF16),
            pltpu.VMEM((16, C * C, 128), BF16),
            pltpu.VMEM((8, 8, 128, 128), BF16),
            dma((3,)), dma((3,)), dma((3, CHUNKS)), dma((3, CHUNKS)), dma((3,)), dma((3,)),
            dma((4, 2)), dma((4, 2)), dma((4, 2)), dma((4, 2)), dma((7,)), dma((7,)),
            dma((3, CHUNKS)), dma((3, CHUNKS)), dma((7,)), dma((7,)), dma((2,)),
        ],
        compiler_params=pltpu.CompilerParams(
            collective_id=0, has_side_effects=True, vmem_limit_bytes=58 * 2**20
        ),
        name="step",
    )(alignment, w_factors.T, query_weight, w_keyval, w_gate, output_weight, w_pair_out)


def place_kernel(update_ref, pair_ref, update_out, pair_out, rows, turned, pieces, *sems):
    row_sems, piece_sems, turned_sems, placed_sem = sems
    x = lax.axis_index("x_hi") * 2 + lax.axis_index("x_lo")
    y, z, core = lax.axis_index("y"), lax.axis_index("z"), lax.axis_index("core")
    row_loads = [
        pltpu.make_async_copy(update_ref.at[n], rows.at[n], row_sems.at[n]) for n in range(4)
    ]
    piece_loads = [
        pltpu.make_async_copy(pair_ref.at[n], pieces.at[n], piece_sems.at[n]) for n in range(8)
    ]
    for load in row_loads + piece_loads:
        load.start()
    copies = []

    def put(piece):
        there_core = flipped(core, piece % 2)
        away = piece // 2
        for step in range(4):
            there_y = lax.rem(y + there_core * away + (1 - there_core) * step, 4)
            there_z = lax.rem(z + there_core * step + (1 - there_core) * away, 4)
            for dx in range(4):
                there_x = lax.rem(x + dx, 4)
                copy = pltpu.make_async_copy(
                    pieces.at[piece, :, step * 4 + dx],
                    pair_out.at[
                        :, lax.rem(there_x, 2), there_y, there_z, there_x // 2, there_core
                    ],
                    placed_sem,
                )
                copy.start()
                copies.append(copy)

    for n in range(4):
        row_loads[n].wait()
        turned[n] = jnp.swapaxes(rows[n].astype(F32), 0, 1).astype(BF16)
        first = pl.multiple_of(seq_of(n) * 8, 8)
        copy = pltpu.make_async_copy(
            turned.at[n], update_out.at[:, pl.ds(first, 8), :], turned_sems.at[n]
        )
        copy.start()
        copies.append(copy)
        for piece in (2 * n, 2 * n + 1):
            piece_loads[piece].wait()
            put(piece)
    for copy in copies:
        copy.wait()


def place_call(update, pieces):
    dma = pltpu.SemaphoreType.DMA
    update, pair = pl.pallas_call(
        place_kernel,
        in_specs=[ANY_SPEC] * 2,
        out_specs=[ANY_SPEC] * 2,
        out_shape=[
            jax.ShapeDtypeStruct((96, 32, 256), BF16),
            jax.ShapeDtypeStruct((8, 2, 4, 4, 2, 2, 8, 128), BF16),
        ],
        scratch_shapes=[
            pltpu.VMEM((4, 8, 96, 256), BF16),
            pltpu.VMEM((4, 96, 8, 256), BF16),
            pltpu.VMEM((8, 8, 16, 8, 128), BF16),
            dma((4,)), dma((8,)), dma((4,)), dma,
        ],
        compiler_params=pltpu.CompilerParams(vmem_limit_bytes=58 * 2**20),
        name="place",
    )(update, pieces.reshape(8, 8, 16, 8, 128))
    return update, pair.reshape(8, 1024, 128)


def per_device(alignment, query_weight, w_keyval, w_gate, output_weight, w_factors, w_pair_out):
    update, pieces = step_call(
        alignment, w_factors, query_weight, w_keyval, w_gate, output_weight, w_pair_out
    )
    return place_call(update, pieces)


def solution(mesh):
    split = Mesh(mesh.devices.reshape(SIZES), AXES)
    in_specs = (P(SEQ, RES, None), P(), P(), P(), P(), P(), P())
    out_specs = (P(SEQ, RES, None), P(AXES, None, None))
    return jax.shard_map(
        per_device, mesh=split, in_specs=in_specs, out_specs=out_specs, check_vma=False
    )
```

```python
import math

import jax
import jax.numpy as jnp
from jax import lax
from jax.experimental import pallas as pl
from jax.experimental.pallas import tpu as pltpu
from jax.sharding import Mesh
from jax.sharding import PartitionSpec as P

HEADS = 8
HC = 32
C = 32
AXES = ("x_lo", "y", "z", "x_hi", "core")
SIZES = (2, 4, 4, 2, 2)
RES = ("x_lo", "y", "z")
SEQ = ("x_hi", "core")
epsilon = 1e-05
NT = (((1,), (1,)), ((), ()))
TN = (((0,), (0,)), ((), ()))
RELS = ((0, 0), (0, 1), (1, 0), (1, 1))
CHUNKS = 4
PER_CHUNK = 8 // CHUNKS
F32 = jnp.float32
BF16 = jnp.bfloat16
VMEM_SPEC = pl.BlockSpec(memory_space=pltpu.VMEM)
ANY_SPEC = pl.BlockSpec(memory_space=pl.ANY)
MESH = pl.DeviceIdType.MESH


def flipped(value, flip):
    return 1 - value if flip else value


def seq_of(rel):
    hi, core = lax.axis_index("x_hi"), lax.axis_index("core")
    return flipped(hi, RELS[rel][0]) * 2 + flipped(core, RELS[rel][1])


def seq_device(rel):
    hi, core = lax.axis_index("x_hi"), lax.axis_index("core")
    return {"x_hi": flipped(hi, RELS[rel][0]), "core": flipped(core, RELS[rel][1])}


def x_device(shift):
    x = lax.axis_index("x_hi") * 2 + lax.axis_index("x_lo")
    there = lax.rem(x + shift + 4, 4)
    return {"x_lo": lax.rem(there, 2), "x_hi": there // 2}


def gather_device(shift, flip=0):
    core = lax.axis_index("core")
    return {
        "y": lax.rem(lax.axis_index("y") + (1 - core) * (shift + 4), 4),
        "z": lax.rem(lax.axis_index("z") + core * (shift + 4), 4),
        "core": flipped(core, flip),
    }


def share_device(shift, flip=0):
    core = lax.axis_index("core")
    return {
        "y": lax.rem(lax.axis_index("y") + core * (shift + 4), 4),
        "z": lax.rem(lax.axis_index("z") + (1 - core) * (shift + 4), 4),
        "core": flipped(core, flip),
    }


def remote(src, dst, send, recv, device):
    return pltpu.make_async_remote_copy(
        src_ref=src, dst_ref=dst, send_sem=send, recv_sem=recv, device_id=device, device_id_type=MESH
    )


def step_kernel(
    x_hbm, wf_hbm, wq_hbm, wkv_hbm, wg_hbm, wo_hbm, wp_hbm,
    update_out, pair_out,
    x_in, wf_ref, wq_ref, wkv_ref, wg_ref, wo_ref, wp_ref, normed_out, rows_in, factors_out, factors_in, rights, lefts, spread_q, w_turned, w_pair,
    update_made, aligned, held, blocks,
    f_send, f_recv, n_send, n_recv, x_send, x_recv, y_send, y_recv, w_send, w_recv,
    l_send, l_recv, u_send, u_recv, p_send, p_recv, own_sem, x_sem, weight_sem, v_send, v_recv,
):
    def x_load(rel):
        first = pl.multiple_of(seq_of(rel) * 8, 8)
        return pltpu.make_async_copy(
            x_hbm.at[:, pl.ds(first, 8), :], x_in.at[rel], x_sem.at[rel]
        )

    weight_loads = [
        pltpu.make_async_copy(src, dst, weight_sem.at[n])
        for n, (src, dst) in enumerate(
            zip(
                (wf_hbm, wq_hbm, wkv_hbm, wg_hbm, wo_hbm, wp_hbm),
                (wf_ref, wq_ref, wkv_ref, wg_ref, wo_ref, wp_ref),
            )
        )
    ]
    x_load(2).start()
    weight_loads[0].start()
    for rel in (3, 1, 0):
        x_load(rel).start()
    for load in weight_loads[1:]:
        load.start()
    barrier = pltpu.get_barrier_semaphore()
    partners = [seq_device(rel) for rel in (1, 2, 3)] + [x_device(1), x_device(-1)]
    partners += [gather_device(1), gather_device(-1)]
    partners += [share_device(shift, flip) for shift in (1, 2, 3) for flip in (0, 1)]
    partners += [gather_device(shift, 1) for shift in (1, 2, 3)]
    for device in partners:
        pl.semaphore_signal(barrier, inc=1, device_id=device, device_id_type=MESH)

    def factor_copy(rel):
        return remote(
            factors_out.at[rel - 1], factors_in.at[seq_of(0)],
            f_send.at[rel - 1], f_recv.at[rel - 1], seq_device(rel),
        )

    def normed_copy(rel, chunk):
        part = pl.ds(chunk * PER_CHUNK, PER_CHUNK)
        return remote(
            normed_out.at[rel - 1, part], rows_in.at[rel, part],
            n_send.at[rel - 1, chunk], n_recv.at[rel - 1, chunk], seq_device(rel),
        )

    def x_copy(dx):
        return remote(
            rights.at[0, 0], rights.at[0, dx], x_send.at[dx - 1], x_recv.at[dx - 1], x_device(-dx)
        )

    def x_relay(way):
        half = pl.ds(16 * way, 16)
        return remote(
            rights.at[0, (1, 3)[way], half], rights.at[0, 2, half],
            v_send.at[way], v_recv.at[way], x_device((-1, 1)[way]),
        )

    def y_copy(dx, way):
        return remote(
            rights.at[0, dx], rights.at[(1, 3)[way], dx],
            y_send.at[dx, way], y_recv.at[dx, way], gather_device((-1, 1)[way]),
        )

    def relay_copy(dx, way):
        half = pl.ds(16 * way, 16)
        return remote(
            rights.at[(1, 3)[way], dx, half], rights.at[2, dx, half],
            w_send.at[dx, way], w_recv.at[dx, way], gather_device((-1, 1)[way]),
        )

    def left_copy(n):
        away, flip = n // 2, n % 2
        device = gather_device(-away, 1) if flip else share_device(-away)
        return remote(
            lefts.at[0, 0], lefts.at[away, flip], l_send.at[n - 1], l_recv.at[n - 1], device
        )

    def update_copy(rel, r):
        return remote(
            update_made.at[rel, r], update_out.at[rel, r],
            u_send.at[rel - 1, r], u_recv.at[rel - 1, r], seq_device(rel),
        )

    def block_copy(n):
        dz, dc = n // 2, n % 2
        there = 2 * ((4 - dz) % 4) + dc
        return remote(
            blocks.at[n], pair_out.at[there], p_send.at[n - 1], p_recv.at[there - 1],
            share_device(dz, dc),
        )

    weight_loads[0].wait()
    weight = wf_ref[...]
    none = jnp.zeros_like(weight)
    even = jnp.concatenate([weight, none], axis=0)
    odd = jnp.concatenate([none, weight], axis=0)
    span = 32
    for rel in (2, 3, 1, 0):
        x_load(rel).wait()
        normed_ref = normed_out.at[rel - 1] if rel else rows_in.at[0]
        factor_ref = factors_out.at[rel - 1] if rel else factors_in.at[seq_of(0)]

        def norm_rows(part, _, rel=rel, normed_ref=normed_ref):
            rows = pl.ds(pl.multiple_of(part * span, span), span)
            x = x_in[rel, rows].astype(F32)
            centered = x - jnp.mean(x, axis=-1, keepdims=True)
            spread = jnp.mean(centered * centered, axis=-1, keepdims=True)
            normed = centered * lax.rsqrt(spread + epsilon)
            normed_ref[:, rows, :] = jnp.swapaxes(normed, 0, 1).astype(BF16)
            return 0

        lax.fori_loop(0, 96 // span, norm_rows, 0, unroll=True)
        for pair in range(4):
            made = lax.dot_general(
                normed_ref[2 * pair], even, NT, preferred_element_type=F32
            ) + lax.dot_general(normed_ref[2 * pair + 1], odd, NT, preferred_element_type=F32)
            factor_ref[:, pair * 128 : (pair + 1) * 128] = made.astype(BF16)
        if rel == 2:
            pl.semaphore_wait(barrier, len(partners))
        if rel:
            factor_copy(rel).start()

    for load in weight_loads[1:]:
        load.wait()
    w_turned[:256] = wq_ref[...].astype(F32).T.astype(BF16)
    w_turned[256:512] = wkv_ref[:, 256:].astype(F32).T.astype(BF16)
    w_turned[512:] = wg_ref[...].astype(F32).T.astype(BF16)
    pair_rows = jnp.swapaxes(wp_ref[...].astype(F32).reshape(C, C, 128), 0, 1)
    w_pair[...] = pair_rows.reshape(C * C, 128).T.astype(BF16)
    spread_q[...] = jnp.zeros_like(spread_q)
    for rel in (2, 3, 1):
        normed_copy(rel, 0).start()

    for rel in (1, 2, 3):
        factor_copy(rel).wait_recv()
    turned = factors_in[...].astype(F32).reshape(384, 512).T.reshape(8, 64, 384)
    rights[0, 0] = jnp.swapaxes(turned[:, C:], 0, 1).astype(BF16)
    lefts[0, 0] = turned[:, :C].reshape(8 * C, 384).astype(BF16)
    for dx in (1, 3):
        x_copy(dx).start()
    for way in (0, 1):
        y_copy(0, way).start()
    for n in range(1, 8):
        left_copy(n).start()

    ones = jnp.ones((16, 384), BF16)
    scale = math.log2(math.e) / math.sqrt(HC)

    def residue(r, slot):
        rows = jnp.concatenate([rows_in[k, r] for k in range(4)], axis=0)
        keys = jnp.dot(rows, wkv_ref[:, :256], preferred_element_type=F32).astype(BF16)
        queries = lax.dot_general(w_turned[:256], rows, NT, preferred_element_type=F32).astype(BF16)
        values = lax.dot_general(
            w_turned[256:512], rows, NT, preferred_element_type=F32
        ).astype(BF16)
        gating = jax.nn.sigmoid(
            lax.dot_general(w_turned[512:], rows, NT, preferred_element_type=F32)
        )
        for h in range(HEADS):
            at = slice(h * HC, (h + 1) * HC)
            spread_q[slot, h // 2, at, (h % 2) * 384 : (h % 2 + 1) * 384] = queries[at]
        gated = []
        for pair in range(HEADS // 2):
            scores = jnp.dot(keys, spread_q[slot, pair], preferred_element_type=F32)
            weights = jnp.exp2(scores * scale).astype(BF16)
            for k in range(2):
                h = 2 * pair + k
                at = slice(h * HC, (h + 1) * HC)
                summed = jnp.dot(
                    jnp.concatenate([values[at], ones], axis=0),
                    weights[:, k * 384 : (k + 1) * 384],
                    preferred_element_type=F32,
                )
                attended = summed[:HC] / summed[HC : HC + 1]
                gated.append((gating[at] * attended).astype(BF16))
        update = lax.dot_general(
            jnp.concatenate(gated, axis=0), wo_ref[...], TN, preferred_element_type=F32
        ).astype(BF16)
        for k in range(4):
            update_made[k, r] = update[k * 96 : (k + 1) * 96]

    def chunk_step(chunk, _):
        for rel in (1, 2, 3):
            normed_copy(rel, chunk).wait_recv()
        for before, ahead in ((0, 1), (1, 3)):

            @pl.when(chunk == before)
            def _(ahead=ahead):
                for rel in (2, 3, 1):
                    normed_copy(rel, ahead).start()

        for k in range(PER_CHUNK):
            residue(chunk * PER_CHUNK + k, k)
        @pl.when(chunk == 0)
        def _():
            for way in (0, 1):
                x_copy((1, 3)[way]).wait_recv()
                x_relay(way).start()
            for dx in (1, 3):
                for way in (0, 1):
                    y_copy(dx, way).start()
            for rel in (2, 3, 1):
                normed_copy(rel, 2).start()
            for way in (0, 1):
                x_relay(way).wait_recv()
            for way in (0, 1):
                y_copy(2, way).start()
            for way in (0, 1):
                y_copy(0, way).wait_recv()
                relay_copy(0, way).start()

        @pl.when(chunk == 1)
        def _():
            for dx in (1, 3, 2):
                for way in (0, 1):
                    y_copy(dx, way).wait_recv()
                    relay_copy(dx, way).start()

        return 0

    lax.fori_loop(0, CHUNKS - 1, chunk_step, 0)
    for r in range(8 - PER_CHUNK):
        for rel in (2, 3, 1):
            update_copy(rel, r).start()

    for dx in range(4):
        for way in (0, 1):
            relay_copy(dx, way).wait_recv()

    def align(e, _):
        aligned[e] = jnp.concatenate(
            [rights[dy, dx, e] for dy in range(4) for dx in range(4)], axis=0
        )
        return 0

    lax.fori_loop(0, C, align, 0, unroll=4)
    for n in range(1, 8):
        left_copy(n).wait_recv()

    def share_tile(dz):
        left = lefts[dz].reshape(512, 384)
        for k in range(C // 2):
            right = aligned[2 * k : 2 * k + 2].reshape(256, 384)
            made = lax.dot_general(left, right, NT, preferred_element_type=F32).astype(BF16)
            for e in range(2):
                at = (2 * k + e) * C
                held[:, at : at + C, :] = made[:, e * 128 : (e + 1) * 128].reshape(16, C, 128)
        for pair in range(8):
            cols = jnp.concatenate([held[2 * pair], held[2 * pair + 1]], axis=1)
            made = jnp.dot(w_pair[...], cols, preferred_element_type=F32) * (1.0 / 384)
            for k in range(2):
                i = 2 * pair + k
                blocks[2 * dz + i // 8, i % 8] = made[:, k * 128 : (k + 1) * 128].T.astype(BF16)
        for n in (2 * dz, 2 * dz + 1):
            if n:
                block_copy(n).start()

    for dz in (2, 1, 3):
        share_tile(dz)

    for rel in (1, 2, 3):
        normed_copy(rel, CHUNKS - 1).wait_recv()

    def last_residue(r, _):
        residue(r, 0)
        for rel in (2, 3, 1):
            update_copy(rel, r).start()
        return 0

    lax.fori_loop(8 - PER_CHUNK, 8, last_residue, 0)
    own_update = pltpu.make_async_copy(update_made.at[0], update_out.at[0], own_sem.at[0])
    own_update.start()
    share_tile(0)
    own_block = pltpu.make_async_copy(blocks.at[0], pair_out.at[0], own_sem.at[1])
    own_block.start()

    for rel in (1, 2, 3):
        factor_copy(rel).wait_send()
        for chunk in range(CHUNKS):
            normed_copy(rel, chunk).wait_send()
        for r in range(8):
            update_copy(rel, r).wait()
    for way in (0, 1):
        x_copy((1, 3)[way]).wait_send()
        x_relay(way).wait_send()
    for dx in range(4):
        for way in (0, 1):
            y_copy(dx, way).wait_send()
            relay_copy(dx, way).wait_send()
    for n in range(1, 8):
        left_copy(n).wait_send()
    own_update.wait()
    own_block.wait()
    for n in range(1, 8):
        block_copy(n).wait()


def step_call(alignment, w_factors, query_weight, w_keyval, w_gate, output_weight, w_pair_out):
    dma = pltpu.SemaphoreType.DMA
    return pl.pallas_call(
        step_kernel,
        in_specs=[ANY_SPEC] * 7,
        out_specs=[ANY_SPEC] * 2,
        out_shape=[
            jax.ShapeDtypeStruct((4, 8, 96, 256), BF16),
            jax.ShapeDtypeStruct((8, 8, 128, 128), BF16),
        ],
        scratch_shapes=[
            pltpu.VMEM((4, 96, 8, 256), BF16),
            pltpu.VMEM((64, 256), BF16),
            pltpu.VMEM((256, 256), BF16),
            pltpu.VMEM((256, 512), BF16),
            pltpu.VMEM((256, 256), BF16),
            pltpu.VMEM((256, 256), BF16),
            pltpu.VMEM((1024, 128), BF16),
            pltpu.VMEM((3, 8, 96, 256), BF16),
            pltpu.VMEM((4, 8, 96, 256), BF16),
            pltpu.VMEM((3, 96, 512), BF16),
            pltpu.VMEM((4, 96, 512), BF16),
            pltpu.VMEM((4, 4, C, 8, 384), BF16),
            pltpu.VMEM((4, 2, 8 * C, 384), BF16),
            pltpu.VMEM((PER_CHUNK, 4, 256, 768), BF16),
            pltpu.VMEM((768, 256), BF16),
            pltpu.VMEM((128, C * C), BF16),
            pltpu.VMEM((4, 8, 96, 256), BF16),
            pltpu.VMEM((C, 128, 384), BF16),
            pltpu.VMEM((16, C * C, 128), BF16),
            pltpu.VMEM((8, 8, 128, 128), BF16),
            dma((3,)), dma((3,)), dma((3, CHUNKS)), dma((3, CHUNKS)), dma((3,)), dma((3,)),
            dma((4, 2)), dma((4, 2)), dma((4, 2)), dma((4, 2)), dma((7,)), dma((7,)),
            dma((3, 8)), dma((3, 8)), dma((7,)), dma((7,)), dma((2,)), dma((4,)), dma((6,)), dma((2,)), dma((2,)),
        ],
        compiler_params=pltpu.CompilerParams(
            collective_id=0, has_side_effects=True, vmem_limit_bytes=58 * 2**20
        ),
        name="step",
    )(alignment, w_factors.T, query_weight, w_keyval, w_gate, output_weight, w_pair_out)


def place_kernel(update_ref, pair_ref, update_out, pair_out, rows, turned, pieces, *sems):
    row_sems, piece_sems, turned_sems, placed_sem = sems
    x = lax.axis_index("x_hi") * 2 + lax.axis_index("x_lo")
    y, z, core = lax.axis_index("y"), lax.axis_index("z"), lax.axis_index("core")
    row_loads = [
        pltpu.make_async_copy(update_ref.at[n], rows.at[n], row_sems.at[n]) for n in range(4)
    ]
    piece_loads = [
        pltpu.make_async_copy(pair_ref.at[n], pieces.at[n], piece_sems.at[n]) for n in range(8)
    ]
    for load in row_loads + piece_loads:
        load.start()
    copies = []

    def put(piece):
        there_core = flipped(core, piece % 2)
        away = piece // 2
        for step in range(4):
            there_y = lax.rem(y + there_core * away + (1 - there_core) * step, 4)
            there_z = lax.rem(z + there_core * step + (1 - there_core) * away, 4)
            for dx in range(4):
                there_x = lax.rem(x + dx, 4)
                copy = pltpu.make_async_copy(
                    pieces.at[piece, :, step * 4 + dx],
                    pair_out.at[
                        :, lax.rem(there_x, 2), there_y, there_z, there_x // 2, there_core
                    ],
                    placed_sem,
                )
                copy.start()
                copies.append(copy)

    for n in range(4):
        row_loads[n].wait()
        turned[n] = jnp.swapaxes(rows[n].astype(F32), 0, 1).astype(BF16)
        first = pl.multiple_of(seq_of(n) * 8, 8)
        copy = pltpu.make_async_copy(
            turned.at[n], update_out.at[:, pl.ds(first, 8), :], turned_sems.at[n]
        )
        copy.start()
        copies.append(copy)
        for piece in (2 * n, 2 * n + 1):
            piece_loads[piece].wait()
            put(piece)
    for copy in copies:
        copy.wait()


def place_call(update, pieces):
    dma = pltpu.SemaphoreType.DMA
    update, pair = pl.pallas_call(
        place_kernel,
        in_specs=[ANY_SPEC] * 2,
        out_specs=[ANY_SPEC] * 2,
        out_shape=[
            jax.ShapeDtypeStruct((96, 32, 256), BF16),
            jax.ShapeDtypeStruct((8, 2, 4, 4, 2, 2, 8, 128), BF16),
        ],
        scratch_shapes=[
            pltpu.VMEM((4, 8, 96, 256), BF16),
            pltpu.VMEM((4, 96, 8, 256), BF16),
            pltpu.VMEM((8, 8, 16, 8, 128), BF16),
            dma((4,)), dma((8,)), dma((4,)), dma,
        ],
        compiler_params=pltpu.CompilerParams(vmem_limit_bytes=58 * 2**20),
        name="place",
    )(update, pieces.reshape(8, 8, 16, 8, 128))
    return update, pair.reshape(8, 1024, 128)


def per_device(alignment, query_weight, w_keyval, w_gate, output_weight, w_factors, w_pair_out):
    update, pieces = step_call(
        alignment, w_factors, query_weight, w_keyval, w_gate, output_weight, w_pair_out
    )
    return place_call(update, pieces)


def solution(mesh):
    split = Mesh(mesh.devices.reshape(SIZES), AXES)
    in_specs = (P(SEQ, RES, None), P(), P(), P(), P(), P(), P())
    out_specs = (P(SEQ, RES, None), P(AXES, None, None))
    return jax.shard_map(
        per_device, mesh=split, in_specs=in_specs, out_specs=out_specs, check_vma=False
    )
```

```python
import math

import jax
import jax.numpy as jnp
from jax import lax
from jax.experimental import pallas as pl
from jax.experimental.pallas import tpu as pltpu
from jax.sharding import Mesh
from jax.sharding import PartitionSpec as P

HEADS = 8
HC = 32
C = 32
AXES = ("x_lo", "y", "z", "x_hi", "core")
SIZES = (2, 4, 4, 2, 2)
RES = ("x_lo", "y", "z")
SEQ = ("x_hi", "core")
epsilon = 1e-05
NT = (((1,), (1,)), ((), ()))
TN = (((0,), (0,)), ((), ()))
RELS = ((0, 0), (0, 1), (1, 0), (1, 1))
CHUNKS = 4
PER_CHUNK = 8 // CHUNKS
AHEAD = 2
F32 = jnp.float32
BF16 = jnp.bfloat16
VMEM_SPEC = pl.BlockSpec(memory_space=pltpu.VMEM)
ANY_SPEC = pl.BlockSpec(memory_space=pl.ANY)
MESH = pl.DeviceIdType.MESH


def flipped(value, flip):
    return 1 - value if flip else value


def seq_of(rel):
    hi, core = lax.axis_index("x_hi"), lax.axis_index("core")
    return flipped(hi, RELS[rel][0]) * 2 + flipped(core, RELS[rel][1])


def seq_device(rel):
    hi, core = lax.axis_index("x_hi"), lax.axis_index("core")
    return {"x_hi": flipped(hi, RELS[rel][0]), "core": flipped(core, RELS[rel][1])}


def x_device(shift):
    x = lax.axis_index("x_hi") * 2 + lax.axis_index("x_lo")
    there = lax.rem(x + shift + 4, 4)
    return {"x_lo": lax.rem(there, 2), "x_hi": there // 2}


def gather_device(shift, flip=0):
    core = lax.axis_index("core")
    return {
        "y": lax.rem(lax.axis_index("y") + (1 - core) * (shift + 4), 4),
        "z": lax.rem(lax.axis_index("z") + core * (shift + 4), 4),
        "core": flipped(core, flip),
    }


def share_device(shift, flip=0):
    core = lax.axis_index("core")
    return {
        "y": lax.rem(lax.axis_index("y") + core * (shift + 4), 4),
        "z": lax.rem(lax.axis_index("z") + (1 - core) * (shift + 4), 4),
        "core": flipped(core, flip),
    }


def remote(src, dst, send, recv, device):
    return pltpu.make_async_remote_copy(
        src_ref=src, dst_ref=dst, send_sem=send, recv_sem=recv, device_id=device, device_id_type=MESH
    )


def step_kernel(
    x_hbm, wf_hbm, wq_hbm, wkv_hbm, wg_hbm, wo_hbm, wp_hbm,
    update_out, pair_out,
    x_in, wf_ref, wq_ref, wkv_ref, wg_ref, wo_ref, wp_ref, normed_out, rows_in, factors_out, factors_in, rights, lefts, spread_q, w_turned, w_pair,
    update_made, aligned, held, blocks,
    f_send, f_recv, n_send, n_recv, x_send, x_recv, y_send, y_recv, w_send, w_recv,
    l_send, l_recv, u_send, u_recv, p_send, p_recv, own_sem, x_sem, weight_sem, v_send, v_recv,
):
    def x_load(rel):
        first = pl.multiple_of(seq_of(rel) * 8, 8)
        return pltpu.make_async_copy(
            x_hbm.at[:, pl.ds(first, 8), :], x_in.at[rel], x_sem.at[rel]
        )

    weight_loads = [
        pltpu.make_async_copy(src, dst, weight_sem.at[n])
        for n, (src, dst) in enumerate(
            zip(
                (wf_hbm, wq_hbm, wkv_hbm, wg_hbm, wo_hbm, wp_hbm),
                (wf_ref, wq_ref, wkv_ref, wg_ref, wo_ref, wp_ref),
            )
        )
    ]
    x_load(2).start()
    weight_loads[0].start()
    for rel in (3, 1, 0):
        x_load(rel).start()
    for load in weight_loads[1:]:
        load.start()
    barrier = pltpu.get_barrier_semaphore()
    partners = [seq_device(rel) for rel in (1, 2, 3)] + [x_device(1), x_device(-1)]
    partners += [gather_device(1), gather_device(-1)]
    partners += [share_device(shift, flip) for shift in (1, 2, 3) for flip in (0, 1)]
    partners += [gather_device(shift, 1) for shift in (1, 2, 3)]
    for device in partners:
        pl.semaphore_signal(barrier, inc=1, device_id=device, device_id_type=MESH)

    def factor_copy(rel):
        return remote(
            factors_out.at[rel - 1], factors_in.at[seq_of(0)],
            f_send.at[rel - 1], f_recv.at[rel - 1], seq_device(rel),
        )

    def normed_copy(rel, chunk):
        part = pl.ds(chunk * PER_CHUNK, PER_CHUNK)
        return remote(
            normed_out.at[rel - 1, part], rows_in.at[rel, part],
            n_send.at[rel - 1, chunk], n_recv.at[rel - 1, chunk], seq_device(rel),
        )

    def x_copy(dx):
        return remote(
            rights.at[0, 0], rights.at[0, dx], x_send.at[dx - 1], x_recv.at[dx - 1], x_device(-dx)
        )

    def x_relay(way):
        half = pl.ds(16 * way, 16)
        return remote(
            rights.at[0, (1, 3)[way], half], rights.at[0, 2, half],
            v_send.at[way], v_recv.at[way], x_device((-1, 1)[way]),
        )

    def y_copy(dx, way):
        return remote(
            rights.at[0, dx], rights.at[(1, 3)[way], dx],
            y_send.at[dx, way], y_recv.at[dx, way], gather_device((-1, 1)[way]),
        )

    def relay_copy(dx, way):
        half = pl.ds(16 * way, 16)
        return remote(
            rights.at[(1, 3)[way], dx, half], rights.at[2, dx, half],
            w_send.at[dx, way], w_recv.at[dx, way], gather_device((-1, 1)[way]),
        )

    def left_copy(n):
        away, flip = n // 2, n % 2
        device = gather_device(-away, 1) if flip else share_device(-away)
        return remote(
            lefts.at[0, 0], lefts.at[away, flip], l_send.at[n - 1], l_recv.at[n - 1], device
        )

    def update_copy(rel, r):
        return remote(
            update_made.at[rel, r], update_out.at[rel, r],
            u_send.at[rel - 1, r], u_recv.at[rel - 1, r], seq_device(rel),
        )

    def block_copy(n):
        dz, dc = n // 2, n % 2
        there = 2 * ((4 - dz) % 4) + dc
        return remote(
            blocks.at[n], pair_out.at[there], p_send.at[n - 1], p_recv.at[there - 1],
            share_device(dz, dc),
        )

    weight_loads[0].wait()
    weight = wf_ref[...]
    none = jnp.zeros_like(weight)
    even = jnp.concatenate([weight, none], axis=0)
    odd = jnp.concatenate([none, weight], axis=0)
    span = 32
    for rel in (2, 3, 1, 0):
        x_load(rel).wait()
        normed_ref = normed_out.at[rel - 1] if rel else rows_in.at[0]
        factor_ref = factors_out.at[rel - 1] if rel else factors_in.at[seq_of(0)]

        def norm_rows(part, _, rel=rel, normed_ref=normed_ref):
            rows = pl.ds(pl.multiple_of(part * span, span), span)
            x = x_in[rel, rows].astype(F32)
            centered = x - jnp.mean(x, axis=-1, keepdims=True)
            spread = jnp.mean(centered * centered, axis=-1, keepdims=True)
            normed = centered * lax.rsqrt(spread + epsilon)
            normed_ref[:, rows, :] = jnp.swapaxes(normed, 0, 1).astype(BF16)
            return 0

        lax.fori_loop(0, 96 // span, norm_rows, 0, unroll=True)
        for pair in range(4):
            made = lax.dot_general(
                normed_ref[2 * pair], even, NT, preferred_element_type=F32
            ) + lax.dot_general(normed_ref[2 * pair + 1], odd, NT, preferred_element_type=F32)
            factor_ref[:, pair * 128 : (pair + 1) * 128] = made.astype(BF16)
        if rel == 2:
            pl.semaphore_wait(barrier, len(partners))
        if rel:
            factor_copy(rel).start()

    for load in weight_loads[1:]:
        load.wait()
    w_turned[:256] = wq_ref[...].astype(F32).T.astype(BF16)
    w_turned[256:512] = wkv_ref[:, 256:].astype(F32).T.astype(BF16)
    w_turned[512:] = wg_ref[...].astype(F32).T.astype(BF16)
    pair_rows = jnp.swapaxes(wp_ref[...].astype(F32).reshape(C, C, 128), 0, 1)
    w_pair[...] = pair_rows.reshape(C * C, 128).T.astype(BF16)
    spread_q[...] = jnp.zeros_like(spread_q)
    for rel in (2, 3, 1):
        normed_copy(rel, 0).start()

    for rel in (1, 2, 3):
        factor_copy(rel).wait_recv()
    turned = factors_in[...].astype(F32).reshape(384, 512).T.reshape(8, 64, 384)
    rights[0, 0] = jnp.swapaxes(turned[:, C:], 0, 1).astype(BF16)
    lefts[0, 0] = turned[:, :C].reshape(8 * C, 384).astype(BF16)
    for dx in (1, 3):
        x_copy(dx).start()
    for way in (0, 1):
        y_copy(0, way).start()
    for n in range(1, 8):
        left_copy(n).start()

    ones = jnp.ones((16, 384), BF16)
    scale = math.log2(math.e) / math.sqrt(HC)

    def project(r, slot):
        rows = jnp.concatenate([rows_in[k, r] for k in range(4)], axis=0)
        queries = lax.dot_general(w_turned[:256], rows, NT, preferred_element_type=F32).astype(BF16)
        for h in range(HEADS):
            at = slice(h * HC, (h + 1) * HC)
            spread_q[slot, h // 2, at, (h % 2) * 384 : (h % 2 + 1) * 384] = queries[at]
        keys = jnp.dot(rows, wkv_ref[:, :256], preferred_element_type=F32).astype(BF16)
        values = lax.dot_general(
            w_turned[256:512], rows, NT, preferred_element_type=F32
        ).astype(BF16)
        gating = jax.nn.sigmoid(
            lax.dot_general(w_turned[512:], rows, NT, preferred_element_type=F32)
        )
        return keys, values, gating

    def score(made, slot, pair):
        scores = jnp.dot(made[0], spread_q[slot, pair], preferred_element_type=F32)
        return jnp.exp2(scores * scale).astype(BF16)

    def gather_pair(made, weights, pair):
        gated = []
        for k in range(2):
            h = 2 * pair + k
            at = slice(h * HC, (h + 1) * HC)
            summed = jnp.dot(
                jnp.concatenate([made[1][at], ones], axis=0),
                weights[:, k * 384 : (k + 1) * 384],
                preferred_element_type=F32,
            )
            attended = summed[:HC] / summed[HC : HC + 1]
            gated.append((made[2][at] * attended).astype(BF16))
        return gated

    def finish(r, gated):
        update = lax.dot_general(
            jnp.concatenate(gated, axis=0), wo_ref[...], TN, preferred_element_type=F32
        ).astype(BF16)
        for k in range(4):
            update_made[k, r] = update[k * 96 : (k + 1) * 96]

    def attend(rows):
        waiting = []
        gated = [[] for _ in rows]

        def drain(left):
            while len(waiting) > left:
                n, made, weights, pair = waiting.pop(0)
                gated[n].extend(gather_pair(made, weights, pair))
                if len(gated[n]) == HEADS:
                    finish(rows[n], gated[n])

        for n, r in enumerate(rows):
            made = project(r, n)
            for pair in range(HEADS // 2):
                waiting.append((n, made, score(made, n, pair), pair))
                drain(AHEAD)
        drain(0)

    def chunk_step(chunk, _):
        for rel in (1, 2, 3):
            normed_copy(rel, chunk).wait_recv()
        for before, ahead in ((0, 1), (1, 3)):

            @pl.when(chunk == before)
            def _(ahead=ahead):
                for rel in (2, 3, 1):
                    normed_copy(rel, ahead).start()

        attend([chunk * PER_CHUNK + k for k in range(PER_CHUNK)])
        @pl.when(chunk == 0)
        def _():
            for way in (0, 1):
                x_copy((1, 3)[way]).wait_recv()
                x_relay(way).start()
            for dx in (1, 3):
                for way in (0, 1):
                    y_copy(dx, way).start()
            for rel in (2, 3, 1):
                normed_copy(rel, 2).start()
            for way in (0, 1):
                x_relay(way).wait_recv()
            for way in (0, 1):
                y_copy(2, way).start()
            for way in (0, 1):
                y_copy(0, way).wait_recv()
                relay_copy(0, way).start()

        @pl.when(chunk == 1)
        def _():
            for dx in (1, 3, 2):
                for way in (0, 1):
                    y_copy(dx, way).wait_recv()
                    relay_copy(dx, way).start()

        return 0

    lax.fori_loop(0, CHUNKS - 1, chunk_step, 0)
    for r in range(8 - PER_CHUNK):
        for rel in (2, 3, 1):
            update_copy(rel, r).start()

    for dx in range(4):
        for way in (0, 1):
            relay_copy(dx, way).wait_recv()

    def align(e, _):
        aligned[e] = jnp.concatenate(
            [rights[dy, dx, e] for dy in range(4) for dx in range(4)], axis=0
        )
        return 0

    lax.fori_loop(0, C, align, 0, unroll=4)
    for n in range(1, 8):
        left_copy(n).wait_recv()

    def share_tile(dz):
        left = lefts[dz].reshape(512, 384)
        for k in range(C // 2):
            right = aligned[2 * k : 2 * k + 2].reshape(256, 384)
            made = lax.dot_general(left, right, NT, preferred_element_type=F32).astype(BF16)
            for e in range(2):
                at = (2 * k + e) * C
                held[:, at : at + C, :] = made[:, e * 128 : (e + 1) * 128].reshape(16, C, 128)
        for pair in range(8):
            cols = jnp.concatenate([held[2 * pair], held[2 * pair + 1]], axis=1)
            made = jnp.dot(w_pair[...], cols, preferred_element_type=F32) * (1.0 / 384)
            for k in range(2):
                i = 2 * pair + k
                blocks[2 * dz + i // 8, i % 8] = made[:, k * 128 : (k + 1) * 128].T.astype(BF16)
        for n in (2 * dz, 2 * dz + 1):
            if n:
                block_copy(n).start()

    for dz in (2, 1, 3):
        share_tile(dz)

    for rel in (1, 2, 3):
        normed_copy(rel, CHUNKS - 1).wait_recv()

    def last_residue(r, _):
        attend([r])
        for rel in (2, 3, 1):
            update_copy(rel, r).start()
        return 0

    lax.fori_loop(8 - PER_CHUNK, 8, last_residue, 0)
    own_update = pltpu.make_async_copy(update_made.at[0], update_out.at[0], own_sem.at[0])
    own_update.start()
    share_tile(0)
    own_block = pltpu.make_async_copy(blocks.at[0], pair_out.at[0], own_sem.at[1])
    own_block.start()

    for rel in (1, 2, 3):
        factor_copy(rel).wait_send()
        for chunk in range(CHUNKS):
            normed_copy(rel, chunk).wait_send()
        for r in range(8):
            update_copy(rel, r).wait()
    for way in (0, 1):
        x_copy((1, 3)[way]).wait_send()
        x_relay(way).wait_send()
    for dx in range(4):
        for way in (0, 1):
            y_copy(dx, way).wait_send()
            relay_copy(dx, way).wait_send()
    for n in range(1, 8):
        left_copy(n).wait_send()
    own_update.wait()
    own_block.wait()
    for n in range(1, 8):
        block_copy(n).wait()


def step_call(alignment, w_factors, query_weight, w_keyval, w_gate, output_weight, w_pair_out):
    dma = pltpu.SemaphoreType.DMA
    return pl.pallas_call(
        step_kernel,
        in_specs=[ANY_SPEC] * 7,
        out_specs=[ANY_SPEC] * 2,
        out_shape=[
            jax.ShapeDtypeStruct((4, 8, 96, 256), BF16),
            jax.ShapeDtypeStruct((8, 8, 128, 128), BF16),
        ],
        scratch_shapes=[
            pltpu.VMEM((4, 96, 8, 256), BF16),
            pltpu.VMEM((64, 256), BF16),
            pltpu.VMEM((256, 256), BF16),
            pltpu.VMEM((256, 512), BF16),
            pltpu.VMEM((256, 256), BF16),
            pltpu.VMEM((256, 256), BF16),
            pltpu.VMEM((1024, 128), BF16),
            pltpu.VMEM((3, 8, 96, 256), BF16),
            pltpu.VMEM((4, 8, 96, 256), BF16),
            pltpu.VMEM((3, 96, 512), BF16),
            pltpu.VMEM((4, 96, 512), BF16),
            pltpu.VMEM((4, 4, C, 8, 384), BF16),
            pltpu.VMEM((4, 2, 8 * C, 384), BF16),
            pltpu.VMEM((PER_CHUNK, 4, 256, 768), BF16),
            pltpu.VMEM((768, 256), BF16),
            pltpu.VMEM((128, C * C), BF16),
            pltpu.VMEM((4, 8, 96, 256), BF16),
            pltpu.VMEM((C, 128, 384), BF16),
            pltpu.VMEM((16, C * C, 128), BF16),
            pltpu.VMEM((8, 8, 128, 128), BF16),
            dma((3,)), dma((3,)), dma((3, CHUNKS)), dma((3, CHUNKS)), dma((3,)), dma((3,)),
            dma((4, 2)), dma((4, 2)), dma((4, 2)), dma((4, 2)), dma((7,)), dma((7,)),
            dma((3, 8)), dma((3, 8)), dma((7,)), dma((7,)), dma((2,)), dma((4,)), dma((6,)), dma((2,)), dma((2,)),
        ],
        compiler_params=pltpu.CompilerParams(
            collective_id=0, has_side_effects=True, vmem_limit_bytes=58 * 2**20
        ),
        name="step",
    )(alignment, w_factors.T, query_weight, w_keyval, w_gate, output_weight, w_pair_out)


def place_kernel(update_ref, pair_ref, update_out, pair_out, rows, turned, pieces, *sems):
    row_sems, piece_sems, turned_sems, placed_sem = sems
    x = lax.axis_index("x_hi") * 2 + lax.axis_index("x_lo")
    y, z, core = lax.axis_index("y"), lax.axis_index("z"), lax.axis_index("core")
    row_loads = [
        pltpu.make_async_copy(update_ref.at[n], rows.at[n], row_sems.at[n]) for n in range(4)
    ]
    piece_loads = [
        pltpu.make_async_copy(pair_ref.at[n], pieces.at[n], piece_sems.at[n]) for n in range(8)
    ]
    for load in row_loads + piece_loads:
        load.start()
    copies = []

    def put(piece):
        there_core = flipped(core, piece % 2)
        away = piece // 2
        for step in range(4):
            there_y = lax.rem(y + there_core * away + (1 - there_core) * step, 4)
            there_z = lax.rem(z + there_core * step + (1 - there_core) * away, 4)
            for dx in range(4):
                there_x = lax.rem(x + dx, 4)
                copy = pltpu.make_async_copy(
                    pieces.at[piece, :, step * 4 + dx],
                    pair_out.at[
                        :, lax.rem(there_x, 2), there_y, there_z, there_x // 2, there_core
                    ],
                    placed_sem,
                )
                copy.start()
                copies.append(copy)

    for n in range(4):
        row_loads[n].wait()
        turned[n] = jnp.swapaxes(rows[n].astype(F32), 0, 1).astype(BF16)
        first = pl.multiple_of(seq_of(n) * 8, 8)
        copy = pltpu.make_async_copy(
            turned.at[n], update_out.at[:, pl.ds(first, 8), :], turned_sems.at[n]
        )
        copy.start()
        copies.append(copy)
        for piece in (2 * n, 2 * n + 1):
            piece_loads[piece].wait()
            put(piece)
    for copy in copies:
        copy.wait()


def place_call(update, pieces):
    dma = pltpu.SemaphoreType.DMA
    update, pair = pl.pallas_call(
        place_kernel,
        in_specs=[ANY_SPEC] * 2,
        out_specs=[ANY_SPEC] * 2,
        out_shape=[
            jax.ShapeDtypeStruct((96, 32, 256), BF16),
            jax.ShapeDtypeStruct((8, 2, 4, 4, 2, 2, 8, 128), BF16),
        ],
        scratch_shapes=[
            pltpu.VMEM((4, 8, 96, 256), BF16),
            pltpu.VMEM((4, 96, 8, 256), BF16),
            pltpu.VMEM((8, 8, 16, 8, 128), BF16),
            dma((4,)), dma((8,)), dma((4,)), dma,
        ],
        compiler_params=pltpu.CompilerParams(vmem_limit_bytes=58 * 2**20),
        name="place",
    )(update, pieces.reshape(8, 8, 16, 8, 128))
    return update, pair.reshape(8, 1024, 128)


def per_device(alignment, query_weight, w_keyval, w_gate, output_weight, w_factors, w_pair_out):
    update, pieces = step_call(
        alignment, w_factors, query_weight, w_keyval, w_gate, output_weight, w_pair_out
    )
    return place_call(update, pieces)


def solution(mesh):
    split = Mesh(mesh.devices.reshape(SIZES), AXES)
    in_specs = (P(SEQ, RES, None), P(), P(), P(), P(), P(), P())
    out_specs = (P(SEQ, RES, None), P(AXES, None, None))
    return jax.shard_map(
        per_device, mesh=split, in_specs=in_specs, out_specs=out_specs, check_vma=False
    )
```

```python
import math

import jax
import jax.numpy as jnp
from jax import lax
from jax.experimental import pallas as pl
from jax.experimental.pallas import tpu as pltpu
from jax.sharding import Mesh
from jax.sharding import PartitionSpec as P

HEADS = 8
HC = 32
C = 32
AXES = ("x_lo", "y", "z", "x_hi", "core")
SIZES = (2, 4, 4, 2, 2)
RES = ("x_lo", "y", "z")
SEQ = ("x_hi", "core")
epsilon = 1e-05
NT = (((1,), (1,)), ((), ()))
TN = (((0,), (0,)), ((), ()))
RELS = ((0, 0), (0, 1), (1, 0), (1, 1))
CHUNKS = 4
PER_CHUNK = 8 // CHUNKS
AHEAD = 2
F32 = jnp.float32
BF16 = jnp.bfloat16
VMEM_SPEC = pl.BlockSpec(memory_space=pltpu.VMEM)
ANY_SPEC = pl.BlockSpec(memory_space=pl.ANY)
MESH = pl.DeviceIdType.MESH


def flipped(value, flip):
    return 1 - value if flip else value


def seq_of(rel):
    hi, core = lax.axis_index("x_hi"), lax.axis_index("core")
    return flipped(hi, RELS[rel][0]) * 2 + flipped(core, RELS[rel][1])


def seq_device(rel):
    hi, core = lax.axis_index("x_hi"), lax.axis_index("core")
    return {"x_hi": flipped(hi, RELS[rel][0]), "core": flipped(core, RELS[rel][1])}


def x_device(shift):
    x = lax.axis_index("x_hi") * 2 + lax.axis_index("x_lo")
    there = lax.rem(x + shift + 4, 4)
    return {"x_lo": lax.rem(there, 2), "x_hi": there // 2}


def gather_device(shift, flip=0):
    core = lax.axis_index("core")
    return {
        "y": lax.rem(lax.axis_index("y") + (1 - core) * (shift + 4), 4),
        "z": lax.rem(lax.axis_index("z") + core * (shift + 4), 4),
        "core": flipped(core, flip),
    }


def share_device(shift, flip=0):
    core = lax.axis_index("core")
    return {
        "y": lax.rem(lax.axis_index("y") + core * (shift + 4), 4),
        "z": lax.rem(lax.axis_index("z") + (1 - core) * (shift + 4), 4),
        "core": flipped(core, flip),
    }


def remote(src, dst, send, recv, device):
    return pltpu.make_async_remote_copy(
        src_ref=src, dst_ref=dst, send_sem=send, recv_sem=recv, device_id=device, device_id_type=MESH
    )


def step_kernel(
    x_hbm, wf_hbm, wq_hbm, wkv_hbm, wg_hbm, wo_hbm, wp_hbm,
    update_out, pair_out,
    x_in, wf_ref, wq_ref, wkv_ref, wg_ref, wo_ref, wp_ref, normed_out, rows_in, factors_out, factors_in, rights, lefts, spread_q, w_turned, w_pair,
    update_made, aligned, held, blocks,
    f_send, f_recv, n_send, n_recv, x_send, x_recv, y_send, y_recv, w_send, w_recv,
    l_send, l_recv, u_send, u_recv, p_send, p_recv, own_sem, x_sem, weight_sem,
):
    def x_load(rel):
        first = pl.multiple_of(seq_of(rel) * 8, 8)
        return pltpu.make_async_copy(
            x_hbm.at[:, pl.ds(first, 8), :], x_in.at[rel], x_sem.at[rel]
        )

    weight_loads = [
        pltpu.make_async_copy(src, dst, weight_sem.at[n])
        for n, (src, dst) in enumerate(
            zip(
                (wf_hbm, wq_hbm, wkv_hbm, wg_hbm, wo_hbm, wp_hbm),
                (wf_ref, wq_ref, wkv_ref, wg_ref, wo_ref, wp_ref),
            )
        )
    ]
    x_load(2).start()
    weight_loads[0].start()
    for rel in (3, 1, 0):
        x_load(rel).start()
    for load in weight_loads[1:]:
        load.start()
    barrier = pltpu.get_barrier_semaphore()
    partners = [seq_device(rel) for rel in (1, 2, 3)] + [x_device(1), x_device(-1)]
    partners += [gather_device(1), gather_device(-1)]
    partners += [share_device(shift, flip) for shift in (1, 2, 3) for flip in (0, 1)]
    partners += [gather_device(shift, 1) for shift in (1, 2, 3)]
    for device in partners:
        pl.semaphore_signal(barrier, inc=1, device_id=device, device_id_type=MESH)

    def factor_copy(rel):
        return remote(
            factors_out.at[rel - 1], factors_in.at[seq_of(0)],
            f_send.at[rel - 1], f_recv.at[rel - 1], seq_device(rel),
        )

    def normed_copy(rel, chunk):
        part = pl.ds(chunk * PER_CHUNK, PER_CHUNK)
        return remote(
            normed_out.at[rel - 1, part], rows_in.at[rel, part],
            n_send.at[rel - 1, chunk], n_recv.at[rel - 1, chunk], seq_device(rel),
        )

    def x_copy(dx):
        return remote(
            rights.at[0, 0], rights.at[0, dx], x_send.at[dx - 1], x_recv.at[dx - 1], x_device(-dx)
        )

    def y_copy(dx, way):
        return remote(
            rights.at[0, dx], rights.at[(1, 3)[way], dx],
            y_send.at[dx, way], y_recv.at[dx, way], gather_device((-1, 1)[way]),
        )

    def relay_copy(dx, way):
        half = pl.ds(16 * way, 16)
        return remote(
            rights.at[(1, 3)[way], dx, half], rights.at[2, dx, half],
            w_send.at[dx, way], w_recv.at[dx, way], gather_device((-1, 1)[way]),
        )

    def left_copy(n):
        away, flip = n // 2, n % 2
        device = gather_device(-away, 1) if flip else share_device(-away)
        return remote(
            lefts.at[0, 0], lefts.at[away, flip], l_send.at[n - 1], l_recv.at[n - 1], device
        )

    def update_copy(rel, r):
        return remote(
            update_made.at[rel, r], update_out.at[rel, r],
            u_send.at[rel - 1, r], u_recv.at[rel - 1, r], seq_device(rel),
        )

    def block_copy(n):
        dz, dc = n // 2, n % 2
        there = 2 * ((4 - dz) % 4) + dc
        return remote(
            blocks.at[n], pair_out.at[there], p_send.at[n - 1], p_recv.at[there - 1],
            share_device(dz, dc),
        )

    weight_loads[0].wait()
    weight = wf_ref[...]
    none = jnp.zeros_like(weight)
    even = jnp.concatenate([weight, none], axis=0)
    odd = jnp.concatenate([none, weight], axis=0)
    span = 32
    for rel in (2, 3, 1, 0):
        x_load(rel).wait()
        normed_ref = normed_out.at[rel - 1] if rel else rows_in.at[0]
        factor_ref = factors_out.at[rel - 1] if rel else factors_in.at[seq_of(0)]

        def norm_rows(part, _, rel=rel, normed_ref=normed_ref):
            rows = pl.ds(pl.multiple_of(part * span, span), span)
            x = x_in[rel, rows].astype(F32)
            centered = x - jnp.mean(x, axis=-1, keepdims=True)
            spread = jnp.mean(centered * centered, axis=-1, keepdims=True)
            normed = centered * lax.rsqrt(spread + epsilon)
            normed_ref[:, rows, :] = jnp.swapaxes(normed, 0, 1).astype(BF16)
            return 0

        lax.fori_loop(0, 96 // span, norm_rows, 0, unroll=True)
        for pair in range(4):
            made = lax.dot_general(
                normed_ref[2 * pair], even, NT, preferred_element_type=F32
            ) + lax.dot_general(normed_ref[2 * pair + 1], odd, NT, preferred_element_type=F32)
            factor_ref[:, pair * 128 : (pair + 1) * 128] = made.astype(BF16)
        if rel == 2:
            pl.semaphore_wait(barrier, len(partners))
        if rel:
            factor_copy(rel).start()

    for load in weight_loads[1:]:
        load.wait()
    w_turned[:256] = wq_ref[...].astype(F32).T.astype(BF16)
    w_turned[256:512] = wkv_ref[:, 256:].astype(F32).T.astype(BF16)
    w_turned[512:] = wg_ref[...].astype(F32).T.astype(BF16)
    pair_rows = jnp.swapaxes(wp_ref[...].astype(F32).reshape(C, C, 128), 0, 1)
    w_pair[...] = pair_rows.reshape(C * C, 128).T.astype(BF16)
    spread_q[...] = jnp.zeros_like(spread_q)
    for rel in (2, 3, 1):
        normed_copy(rel, 0).start()

    for rel in (1, 2, 3):
        factor_copy(rel).wait_recv()
    turned = factors_in[...].astype(F32).reshape(384, 512).T.reshape(8, 64, 384)
    rights[0, 0] = jnp.swapaxes(turned[:, C:], 0, 1).astype(BF16)
    lefts[0, 0] = turned[:, :C].reshape(8 * C, 384).astype(BF16)
    for dx in (1, 3, 2):
        x_copy(dx).start()
    for way in (0, 1):
        y_copy(0, way).start()
    for n in range(1, 8):
        left_copy(n).start()

    ones = jnp.ones((16, 384), BF16)
    scale = math.log2(math.e) / math.sqrt(HC)

    def project(r, slot):
        rows = jnp.concatenate([rows_in[k, r] for k in range(4)], axis=0)
        queries = lax.dot_general(w_turned[:256], rows, NT, preferred_element_type=F32).astype(BF16)
        for h in range(HEADS):
            at = slice(h * HC, (h + 1) * HC)
            spread_q[slot, h // 2, at, (h % 2) * 384 : (h % 2 + 1) * 384] = queries[at]
        keys = jnp.dot(rows, wkv_ref[:, :256], preferred_element_type=F32).astype(BF16)
        values = lax.dot_general(
            w_turned[256:512], rows, NT, preferred_element_type=F32
        ).astype(BF16)
        gating = jax.nn.sigmoid(
            lax.dot_general(w_turned[512:], rows, NT, preferred_element_type=F32)
        )
        return keys, values, gating

    def score(made, slot, pair):
        scores = jnp.dot(made[0], spread_q[slot, pair], preferred_element_type=F32)
        return jnp.exp2(scores * scale).astype(BF16)

    def gather_pair(made, weights, pair):
        gated = []
        for k in range(2):
            h = 2 * pair + k
            at = slice(h * HC, (h + 1) * HC)
            summed = jnp.dot(
                jnp.concatenate([made[1][at], ones], axis=0),
                weights[:, k * 384 : (k + 1) * 384],
                preferred_element_type=F32,
            )
            attended = summed[:HC] / summed[HC : HC + 1]
            gated.append((made[2][at] * attended).astype(BF16))
        return gated

    def finish(r, gated):
        update = lax.dot_general(
            jnp.concatenate(gated, axis=0), wo_ref[...], TN, preferred_element_type=F32
        ).astype(BF16)
        for k in range(4):
            update_made[k, r] = update[k * 96 : (k + 1) * 96]

    def attend(rows):
        waiting = []
        gated = [[] for _ in rows]

        def drain(left):
            while len(waiting) > left:
                n, made, weights, pair = waiting.pop(0)
                gated[n].extend(gather_pair(made, weights, pair))
                if len(gated[n]) == HEADS:
                    finish(rows[n], gated[n])

        for n, r in enumerate(rows):
            made = project(r, n)
            for pair in range(HEADS // 2):
                waiting.append((n, made, score(made, n, pair), pair))
                drain(AHEAD)
        drain(0)

    def chunk_step(chunk, _):
        for rel in (1, 2, 3):
            normed_copy(rel, chunk).wait_recv()
        for before, ahead in ((0, 1), (2, 3)):

            @pl.when(chunk == before)
            def _(ahead=ahead):
                for rel in (2, 3, 1):
                    normed_copy(rel, ahead).start()

        attend([chunk * PER_CHUNK + k for k in range(PER_CHUNK)])
        @pl.when(chunk == 0)
        def _():
            for way in (0, 1):
                x_copy((1, 3)[way]).wait_recv()
            for dx in (1, 3):
                for way in (0, 1):
                    y_copy(dx, way).start()
            x_copy(2).wait_recv()
            for way in (0, 1):
                y_copy(2, way).start()
            for rel in (2, 3, 1):
                normed_copy(rel, 2).start()
            for dx in (0, 1, 3):
                for way in (0, 1):
                    y_copy(dx, way).wait_recv()
                    relay_copy(dx, way).start()

        @pl.when(chunk == 1)
        def _():
            for way in (0, 1):
                y_copy(2, way).wait_recv()
                relay_copy(2, way).start()

        return 0

    lax.fori_loop(0, CHUNKS - 1, chunk_step, 0)
    for r in range(8 - PER_CHUNK):
        for rel in (2, 3, 1):
            update_copy(rel, r).start()

    for dx in range(4):
        for way in (0, 1):
            relay_copy(dx, way).wait_recv()

    def align(e, _):
        aligned[e] = jnp.concatenate(
            [rights[dy, dx, e] for dy in range(4) for dx in range(4)], axis=0
        )
        return 0

    lax.fori_loop(0, C, align, 0, unroll=4)
    for n in range(1, 8):
        left_copy(n).wait_recv()

    def share_tile(dz):
        left = lefts[dz].reshape(512, 384)
        for k in range(C // 2):
            right = aligned[2 * k : 2 * k + 2].reshape(256, 384)
            made = lax.dot_general(left, right, NT, preferred_element_type=F32).astype(BF16)
            for e in range(2):
                at = (2 * k + e) * C
                held[:, at : at + C, :] = made[:, e * 128 : (e + 1) * 128].reshape(16, C, 128)
        for pair in range(8):
            cols = jnp.concatenate([held[2 * pair], held[2 * pair + 1]], axis=1)
            made = jnp.dot(w_pair[...], cols, preferred_element_type=F32) * (1.0 / 384)
            for k in range(2):
                i = 2 * pair + k
                blocks[2 * dz + i // 8, i % 8] = made[:, k * 128 : (k + 1) * 128].T.astype(BF16)
        for n in (2 * dz, 2 * dz + 1):
            if n:
                block_copy(n).start()

    for dz in (2, 1, 3):
        share_tile(dz)

    for rel in (1, 2, 3):
        normed_copy(rel, CHUNKS - 1).wait_recv()

    def last_residue(r, _):
        attend([r])
        for rel in (2, 3, 1):
            update_copy(rel, r).start()
        return 0

    lax.fori_loop(8 - PER_CHUNK, 8, last_residue, 0)
    own_update = pltpu.make_async_copy(update_made.at[0], update_out.at[0], own_sem.at[0])
    own_update.start()
    share_tile(0)
    own_block = pltpu.make_async_copy(blocks.at[0], pair_out.at[0], own_sem.at[1])
    own_block.start()

    for rel in (1, 2, 3):
        factor_copy(rel).wait_send()
        for chunk in range(CHUNKS):
            normed_copy(rel, chunk).wait_send()
        for r in range(8):
            update_copy(rel, r).wait()
    for dx in (1, 2, 3):
        x_copy(dx).wait_send()
    for dx in range(4):
        for way in (0, 1):
            y_copy(dx, way).wait_send()
            relay_copy(dx, way).wait_send()
    for n in range(1, 8):
        left_copy(n).wait_send()
    own_update.wait()
    own_block.wait()
    for n in range(1, 8):
        block_copy(n).wait()


def step_call(alignment, w_factors, query_weight, w_keyval, w_gate, output_weight, w_pair_out):
    dma = pltpu.SemaphoreType.DMA
    return pl.pallas_call(
        step_kernel,
        in_specs=[ANY_SPEC] * 7,
        out_specs=[ANY_SPEC] * 2,
        out_shape=[
            jax.ShapeDtypeStruct((4, 8, 96, 256), BF16),
            jax.ShapeDtypeStruct((8, 8, 128, 128), BF16),
        ],
        scratch_shapes=[
            pltpu.VMEM((4, 96, 8, 256), BF16),
            pltpu.VMEM((64, 256), BF16),
            pltpu.VMEM((256, 256), BF16),
            pltpu.VMEM((256, 512), BF16),
            pltpu.VMEM((256, 256), BF16),
            pltpu.VMEM((256, 256), BF16),
            pltpu.VMEM((1024, 128), BF16),
            pltpu.VMEM((3, 8, 96, 256), BF16),
            pltpu.VMEM((4, 8, 96, 256), BF16),
            pltpu.VMEM((3, 96, 512), BF16),
            pltpu.VMEM((4, 96, 512), BF16),
            pltpu.VMEM((4, 4, C, 8, 384), BF16),
            pltpu.VMEM((4, 2, 8 * C, 384), BF16),
            pltpu.VMEM((PER_CHUNK, 4, 256, 768), BF16),
            pltpu.VMEM((768, 256), BF16),
            pltpu.VMEM((128, C * C), BF16),
            pltpu.VMEM((4, 8, 96, 256), BF16),
            pltpu.VMEM((C, 128, 384), BF16),
            pltpu.VMEM((16, C * C, 128), BF16),
            pltpu.VMEM((8, 8, 128, 128), BF16),
            dma((3,)), dma((3,)), dma((3, CHUNKS)), dma((3, CHUNKS)), dma((3,)), dma((3,)),
            dma((4, 2)), dma((4, 2)), dma((4, 2)), dma((4, 2)), dma((7,)), dma((7,)),
            dma((3, 8)), dma((3, 8)), dma((7,)), dma((7,)), dma((2,)), dma((4,)), dma((6,)),
        ],
        compiler_params=pltpu.CompilerParams(
            collective_id=0, has_side_effects=True, vmem_limit_bytes=58 * 2**20
        ),
        name="step",
    )(alignment, w_factors.T, query_weight, w_keyval, w_gate, output_weight, w_pair_out)


def place_kernel(update_ref, pair_ref, update_out, pair_out, rows, turned, pieces, *sems):
    row_sems, piece_sems, turned_sems, placed_sem = sems
    x = lax.axis_index("x_hi") * 2 + lax.axis_index("x_lo")
    y, z, core = lax.axis_index("y"), lax.axis_index("z"), lax.axis_index("core")
    row_loads = [
        pltpu.make_async_copy(update_ref.at[n], rows.at[n], row_sems.at[n]) for n in range(4)
    ]
    piece_loads = [
        pltpu.make_async_copy(pair_ref.at[n], pieces.at[n], piece_sems.at[n]) for n in range(8)
    ]
    for load in row_loads + piece_loads:
        load.start()
    copies = []

    def put(piece):
        there_core = flipped(core, piece % 2)
        away = piece // 2
        for step in range(4):
            there_y = lax.rem(y + there_core * away + (1 - there_core) * step, 4)
            there_z = lax.rem(z + there_core * step + (1 - there_core) * away, 4)
            for dx in range(4):
                there_x = lax.rem(x + dx, 4)
                copy = pltpu.make_async_copy(
                    pieces.at[piece, :, step * 4 + dx],
                    pair_out.at[
                        :, lax.rem(there_x, 2), there_y, there_z, there_x // 2, there_core
                    ],
                    placed_sem,
                )
                copy.start()
                copies.append(copy)

    for n in range(4):
        row_loads[n].wait()
        turned[n] = jnp.swapaxes(rows[n].astype(F32), 0, 1).astype(BF16)
        first = pl.multiple_of(seq_of(n) * 8, 8)
        copy = pltpu.make_async_copy(
            turned.at[n], update_out.at[:, pl.ds(first, 8), :], turned_sems.at[n]
        )
        copy.start()
        copies.append(copy)
        for piece in (2 * n, 2 * n + 1):
            piece_loads[piece].wait()
            put(piece)
    for copy in copies:
        copy.wait()


def place_call(update, pieces):
    dma = pltpu.SemaphoreType.DMA
    update, pair = pl.pallas_call(
        place_kernel,
        in_specs=[ANY_SPEC] * 2,
        out_specs=[ANY_SPEC] * 2,
        out_shape=[
            jax.ShapeDtypeStruct((96, 32, 256), BF16),
            jax.ShapeDtypeStruct((8, 2, 4, 4, 2, 2, 8, 128), BF16),
        ],
        scratch_shapes=[
            pltpu.VMEM((4, 8, 96, 256), BF16),
            pltpu.VMEM((4, 96, 8, 256), BF16),
            pltpu.VMEM((8, 8, 16, 8, 128), BF16),
            dma((4,)), dma((8,)), dma((4,)), dma,
        ],
        compiler_params=pltpu.CompilerParams(vmem_limit_bytes=58 * 2**20),
        name="place",
    )(update, pieces.reshape(8, 8, 16, 8, 128))
    return update, pair.reshape(8, 1024, 128)


def per_device(alignment, query_weight, w_keyval, w_gate, output_weight, w_factors, w_pair_out):
    update, pieces = step_call(
        alignment, w_factors, query_weight, w_keyval, w_gate, output_weight, w_pair_out
    )
    return place_call(update, pieces)


def solution(mesh):
    split = Mesh(mesh.devices.reshape(SIZES), AXES)
    in_specs = (P(SEQ, RES, None), P(), P(), P(), P(), P(), P())
    out_specs = (P(SEQ, RES, None), P(AXES, None, None))
    return jax.shard_map(
        per_device, mesh=split, in_specs=in_specs, out_specs=out_specs, check_vma=False
    )
```

```python
import math

import jax
import jax.numpy as jnp
from jax import lax
from jax.experimental import pallas as pl
from jax.experimental.pallas import tpu as pltpu
from jax.sharding import Mesh
from jax.sharding import PartitionSpec as P

HEADS = 8
HC = 32
C = 32
AXES = ("x_lo", "y", "z", "x_hi", "core")
SIZES = (2, 4, 4, 2, 2)
RES = ("x_lo", "y", "z")
SEQ = ("x_hi", "core")
epsilon = 1e-05
NT = (((1,), (1,)), ((), ()))
TN = (((0,), (0,)), ((), ()))
RELS = ((0, 0), (0, 1), (1, 0), (1, 1))
CHUNKS = 4
PER_CHUNK = 8 // CHUNKS
AHEAD = 2
F32 = jnp.float32
BF16 = jnp.bfloat16
VMEM_SPEC = pl.BlockSpec(memory_space=pltpu.VMEM)
ANY_SPEC = pl.BlockSpec(memory_space=pl.ANY)
MESH = pl.DeviceIdType.MESH


def flipped(value, flip):
    return 1 - value if flip else value


def seq_of(rel):
    hi, core = lax.axis_index("x_hi"), lax.axis_index("core")
    return flipped(hi, RELS[rel][0]) * 2 + flipped(core, RELS[rel][1])


def seq_device(rel):
    hi, core = lax.axis_index("x_hi"), lax.axis_index("core")
    return {"x_hi": flipped(hi, RELS[rel][0]), "core": flipped(core, RELS[rel][1])}


def x_device(shift):
    x = lax.axis_index("x_hi") * 2 + lax.axis_index("x_lo")
    there = lax.rem(x + shift + 4, 4)
    return {"x_lo": lax.rem(there, 2), "x_hi": there // 2}


def gather_device(shift, flip=0):
    core = lax.axis_index("core")
    return {
        "y": lax.rem(lax.axis_index("y") + (1 - core) * (shift + 4), 4),
        "z": lax.rem(lax.axis_index("z") + core * (shift + 4), 4),
        "core": flipped(core, flip),
    }


def share_device(shift, flip=0):
    core = lax.axis_index("core")
    return {
        "y": lax.rem(lax.axis_index("y") + core * (shift + 4), 4),
        "z": lax.rem(lax.axis_index("z") + (1 - core) * (shift + 4), 4),
        "core": flipped(core, flip),
    }


def remote(src, dst, send, recv, device):
    return pltpu.make_async_remote_copy(
        src_ref=src, dst_ref=dst, send_sem=send, recv_sem=recv, device_id=device, device_id_type=MESH
    )


def step_kernel(
    x_hbm, wf_hbm, wq_hbm, wkv_hbm, wg_hbm, wo_hbm, wp_hbm,
    update_out, pair_out,
    x_in, wf_ref, wq_ref, wkv_ref, wg_ref, wo_ref, wp_ref, normed_out, rows_in, factors_out, factors_in, rights, lefts, spread_q, w_turned, w_pair,
    update_made, aligned, held, blocks,
    f_send, f_recv, n_send, n_recv, x_send, x_recv, y_send, y_recv, w_send, w_recv,
    l_send, l_recv, u_send, u_recv, p_send, p_recv, own_sem, x_sem, weight_sem, v_send, v_recv,
):
    def x_load(rel):
        first = pl.multiple_of(seq_of(rel) * 8, 8)
        return pltpu.make_async_copy(
            x_hbm.at[:, pl.ds(first, 8), :], x_in.at[rel], x_sem.at[rel]
        )

    weight_loads = [
        pltpu.make_async_copy(src, dst, weight_sem.at[n])
        for n, (src, dst) in enumerate(
            zip(
                (wf_hbm, wq_hbm, wkv_hbm, wg_hbm, wo_hbm, wp_hbm),
                (wf_ref, wq_ref, wkv_ref, wg_ref, wo_ref, wp_ref),
            )
        )
    ]
    x_load(2).start()
    weight_loads[0].start()
    for rel in (3, 1, 0):
        x_load(rel).start()
    for load in weight_loads[1:]:
        load.start()
    barrier = pltpu.get_barrier_semaphore()
    partners = [seq_device(rel) for rel in (1, 2, 3)] + [x_device(1), x_device(-1)]
    partners += [gather_device(1), gather_device(-1)]
    partners += [share_device(shift, flip) for shift in (1, 2, 3) for flip in (0, 1)]
    partners += [gather_device(shift, 1) for shift in (1, 2, 3)]
    for device in partners:
        pl.semaphore_signal(barrier, inc=1, device_id=device, device_id_type=MESH)

    def factor_copy(rel):
        return remote(
            factors_out.at[rel - 1], factors_in.at[seq_of(0)],
            f_send.at[rel - 1], f_recv.at[rel - 1], seq_device(rel),
        )

    def normed_copy(rel, chunk):
        part = pl.ds(chunk * PER_CHUNK, PER_CHUNK)
        return remote(
            normed_out.at[rel - 1, part], rows_in.at[rel, part],
            n_send.at[rel - 1, chunk], n_recv.at[rel - 1, chunk], seq_device(rel),
        )

    def x_copy(dx):
        return remote(
            rights.at[0, 0], rights.at[0, dx], x_send.at[dx - 1], x_recv.at[dx - 1], x_device(-dx)
        )

    def x_relay(way):
        half = pl.ds(16 * way, 16)
        return remote(
            rights.at[0, (1, 3)[way], half], rights.at[0, 2, half],
            v_send.at[way], v_recv.at[way], x_device((-1, 1)[way]),
        )

    def y_copy(dx, way):
        return remote(
            rights.at[0, dx], rights.at[(1, 3)[way], dx],
            y_send.at[dx, way], y_recv.at[dx, way], gather_device((-1, 1)[way]),
        )

    def relay_copy(dx, way):
        half = pl.ds(16 * way, 16)
        return remote(
            rights.at[(1, 3)[way], dx, half], rights.at[2, dx, half],
            w_send.at[dx, way], w_recv.at[dx, way], gather_device((-1, 1)[way]),
        )

    def left_copy(n):
        away, flip = n // 2, n % 2
        device = gather_device(-away, 1) if flip else share_device(-away)
        return remote(
            lefts.at[0, 0], lefts.at[away, flip], l_send.at[n - 1], l_recv.at[n - 1], device
        )

    def update_copy(rel, r):
        return remote(
            update_made.at[rel, r], update_out.at[rel, r],
            u_send.at[rel - 1, r], u_recv.at[rel - 1, r], seq_device(rel),
        )

    def block_copy(n):
        dz, dc = n // 2, n % 2
        there = 2 * ((4 - dz) % 4) + dc
        return remote(
            blocks.at[n], pair_out.at[there], p_send.at[n - 1], p_recv.at[there - 1],
            share_device(dz, dc),
        )

    weight_loads[0].wait()
    weight = wf_ref[...]
    none = jnp.zeros_like(weight)
    even = jnp.concatenate([weight, none], axis=0)
    odd = jnp.concatenate([none, weight], axis=0)
    span = 32
    for rel in (2, 3, 1, 0):
        x_load(rel).wait()
        normed_ref = normed_out.at[rel - 1] if rel else rows_in.at[0]
        factor_ref = factors_out.at[rel - 1] if rel else factors_in.at[seq_of(0)]

        def norm_rows(part, _, rel=rel, normed_ref=normed_ref):
            rows = pl.ds(pl.multiple_of(part * span, span), span)
            x = x_in[rel, rows].astype(F32)
            centered = x - jnp.mean(x, axis=-1, keepdims=True)
            spread = jnp.mean(centered * centered, axis=-1, keepdims=True)
            normed = centered * lax.rsqrt(spread + epsilon)
            normed_ref[:, rows, :] = jnp.swapaxes(normed, 0, 1).astype(BF16)
            return 0

        lax.fori_loop(0, 96 // span, norm_rows, 0, unroll=True)
        for pair in range(4):
            made = lax.dot_general(
                normed_ref[2 * pair], even, NT, preferred_element_type=F32
            ) + lax.dot_general(normed_ref[2 * pair + 1], odd, NT, preferred_element_type=F32)
            factor_ref[:, pair * 128 : (pair + 1) * 128] = made.astype(BF16)
        if rel == 2:
            pl.semaphore_wait(barrier, len(partners))
        if rel:
            factor_copy(rel).start()

    for load in weight_loads[1:]:
        load.wait()
    w_turned[:256] = wq_ref[...].astype(F32).T.astype(BF16)
    w_turned[256:512] = wkv_ref[:, 256:].astype(F32).T.astype(BF16)
    w_turned[512:] = wg_ref[...].astype(F32).T.astype(BF16)
    pair_rows = jnp.swapaxes(wp_ref[...].astype(F32).reshape(C, C, 128), 0, 1)
    w_pair[...] = pair_rows.reshape(C * C, 128).T.astype(BF16)
    spread_q[...] = jnp.zeros_like(spread_q)
    for rel in (2, 3, 1):
        normed_copy(rel, 0).start()

    for rel in (1, 2, 3):
        factor_copy(rel).wait_recv()
    turned = factors_in[...].astype(F32).reshape(384, 512).T.reshape(8, 64, 384)
    rights[0, 0] = jnp.swapaxes(turned[:, C:], 0, 1).astype(BF16)
    lefts[0, 0] = turned[:, :C].reshape(8 * C, 384).astype(BF16)
    for dx in (1, 3):
        x_copy(dx).start()
    for way in (0, 1):
        y_copy(0, way).start()
    for n in range(1, 8):
        left_copy(n).start()

    ones = jnp.ones((16, 384), BF16)
    scale = math.log2(math.e) / math.sqrt(HC)

    def project(r, slot):
        rows = jnp.concatenate([rows_in[k, r] for k in range(4)], axis=0)
        queries = lax.dot_general(w_turned[:256], rows, NT, preferred_element_type=F32).astype(BF16)
        for h in range(HEADS):
            at = slice(h * HC, (h + 1) * HC)
            spread_q[slot, h // 2, at, (h % 2) * 384 : (h % 2 + 1) * 384] = queries[at]
        keys = jnp.dot(rows, wkv_ref[:, :256], preferred_element_type=F32).astype(BF16)
        values = lax.dot_general(
            w_turned[256:512], rows, NT, preferred_element_type=F32
        ).astype(BF16)
        gating = jax.nn.sigmoid(
            lax.dot_general(w_turned[512:], rows, NT, preferred_element_type=F32)
        )
        return keys, values, gating

    def score(made, slot, pair):
        scores = jnp.dot(made[0], spread_q[slot, pair], preferred_element_type=F32)
        return jnp.exp2(scores * scale).astype(BF16)

    def gather_pair(made, weights, pair):
        gated = []
        for k in range(2):
            h = 2 * pair + k
            at = slice(h * HC, (h + 1) * HC)
            summed = jnp.dot(
                jnp.concatenate([made[1][at], ones], axis=0),
                weights[:, k * 384 : (k + 1) * 384],
                preferred_element_type=F32,
            )
            attended = summed[:HC] / summed[HC : HC + 1]
            gated.append((made[2][at] * attended).astype(BF16))
        return gated

    def finish(r, gated):
        update = lax.dot_general(
            jnp.concatenate(gated, axis=0), wo_ref[...], TN, preferred_element_type=F32
        ).astype(BF16)
        for k in range(4):
            update_made[k, r] = update[k * 96 : (k + 1) * 96]

    def attend(rows):
        waiting = []
        gated = [[] for _ in rows]

        def drain(left):
            while len(waiting) > left:
                n, made, weights, pair = waiting.pop(0)
                gated[n].extend(gather_pair(made, weights, pair))
                if len(gated[n]) == HEADS:
                    finish(rows[n], gated[n])

        for n, r in enumerate(rows):
            made = project(r, n)
            for pair in range(HEADS // 2):
                waiting.append((n, made, score(made, n, pair), pair))
                drain(AHEAD)
        drain(0)

    def chunk_step(chunk, _):
        for rel in (1, 2, 3):
            normed_copy(rel, chunk).wait_recv()
        for before, ahead in ((0, 1), (2, 3)):

            @pl.when(chunk == before)
            def _(ahead=ahead):
                for rel in (2, 3, 1):
                    normed_copy(rel, ahead).start()

        attend([chunk * PER_CHUNK + k for k in range(PER_CHUNK)])
        @pl.when(chunk == 0)
        def _():
            for way in (0, 1):
                x_copy((1, 3)[way]).wait_recv()
                x_relay(way).start()
            for dx in (1, 3):
                for way in (0, 1):
                    y_copy(dx, way).start()
            for rel in (2, 3, 1):
                normed_copy(rel, 2).start()
            for way in (0, 1):
                x_relay(way).wait_recv()
            for way in (0, 1):
                y_copy(2, way).start()
            for way in (0, 1):
                y_copy(0, way).wait_recv()
                relay_copy(0, way).start()

        @pl.when(chunk == 1)
        def _():
            for dx in (1, 3):
                for way in (0, 1):
                    y_copy(dx, way).wait_recv()
                    relay_copy(dx, way).start()

        @pl.when(chunk == 2)
        def _():
            for way in (0, 1):
                y_copy(2, way).wait_recv()
                relay_copy(2, way).start()

        return 0

    lax.fori_loop(0, CHUNKS - 1, chunk_step, 0)
    for r in range(8 - PER_CHUNK):
        for rel in (2, 3, 1):
            update_copy(rel, r).start()

    for dx in range(4):
        for way in (0, 1):
            relay_copy(dx, way).wait_recv()

    def align(e, _):
        aligned[e] = jnp.concatenate(
            [rights[dy, dx, e] for dy in range(4) for dx in range(4)], axis=0
        )
        return 0

    lax.fori_loop(0, C, align, 0, unroll=4)
    for n in range(1, 8):
        left_copy(n).wait_recv()

    def share_tile(dz):
        left = lefts[dz].reshape(512, 384)
        for k in range(C // 2):
            right = aligned[2 * k : 2 * k + 2].reshape(256, 384)
            made = lax.dot_general(left, right, NT, preferred_element_type=F32).astype(BF16)
            for e in range(2):
                at = (2 * k + e) * C
                held[:, at : at + C, :] = made[:, e * 128 : (e + 1) * 128].reshape(16, C, 128)
        for pair in range(8):
            cols = jnp.concatenate([held[2 * pair], held[2 * pair + 1]], axis=1)
            made = jnp.dot(w_pair[...], cols, preferred_element_type=F32) * (1.0 / 384)
            for k in range(2):
                i = 2 * pair + k
                blocks[2 * dz + i // 8, i % 8] = made[:, k * 128 : (k + 1) * 128].T.astype(BF16)
        for n in (2 * dz, 2 * dz + 1):
            if n:
                block_copy(n).start()

    for dz in (2, 1, 3):
        share_tile(dz)

    for rel in (1, 2, 3):
        normed_copy(rel, CHUNKS - 1).wait_recv()

    def last_residue(r, _):
        attend([r])
        for rel in (2, 3, 1):
            update_copy(rel, r).start()
        return 0

    lax.fori_loop(8 - PER_CHUNK, 8, last_residue, 0)
    own_update = pltpu.make_async_copy(update_made.at[0], update_out.at[0], own_sem.at[0])
    own_update.start()
    share_tile(0)
    own_block = pltpu.make_async_copy(blocks.at[0], pair_out.at[0], own_sem.at[1])
    own_block.start()

    for rel in (1, 2, 3):
        factor_copy(rel).wait_send()
        for chunk in range(CHUNKS):
            normed_copy(rel, chunk).wait_send()
        for r in range(8):
            update_copy(rel, r).wait()
    for way in (0, 1):
        x_copy((1, 3)[way]).wait_send()
        x_relay(way).wait_send()
    for dx in range(4):
        for way in (0, 1):
            y_copy(dx, way).wait_send()
            relay_copy(dx, way).wait_send()
    for n in range(1, 8):
        left_copy(n).wait_send()
    own_update.wait()
    own_block.wait()
    for n in range(1, 8):
        block_copy(n).wait()


def step_call(alignment, w_factors, query_weight, w_keyval, w_gate, output_weight, w_pair_out):
    dma = pltpu.SemaphoreType.DMA
    return pl.pallas_call(
        step_kernel,
        in_specs=[ANY_SPEC] * 7,
        out_specs=[ANY_SPEC] * 2,
        out_shape=[
            jax.ShapeDtypeStruct((4, 8, 96, 256), BF16),
            jax.ShapeDtypeStruct((8, 8, 128, 128), BF16),
        ],
        scratch_shapes=[
            pltpu.VMEM((4, 96, 8, 256), BF16),
            pltpu.VMEM((64, 256), BF16),
            pltpu.VMEM((256, 256), BF16),
            pltpu.VMEM((256, 512), BF16),
            pltpu.VMEM((256, 256), BF16),
            pltpu.VMEM((256, 256), BF16),
            pltpu.VMEM((1024, 128), BF16),
            pltpu.VMEM((3, 8, 96, 256), BF16),
            pltpu.VMEM((4, 8, 96, 256), BF16),
            pltpu.VMEM((3, 96, 512), BF16),
            pltpu.VMEM((4, 96, 512), BF16),
            pltpu.VMEM((4, 4, C, 8, 384), BF16),
            pltpu.VMEM((4, 2, 8 * C, 384), BF16),
            pltpu.VMEM((PER_CHUNK, 4, 256, 768), BF16),
            pltpu.VMEM((768, 256), BF16),
            pltpu.VMEM((128, C * C), BF16),
            pltpu.VMEM((4, 8, 96, 256), BF16),
            pltpu.VMEM((C, 128, 384), BF16),
            pltpu.VMEM((16, C * C, 128), BF16),
            pltpu.VMEM((8, 8, 128, 128), BF16),
            dma((3,)), dma((3,)), dma((3, CHUNKS)), dma((3, CHUNKS)), dma((3,)), dma((3,)),
            dma((4, 2)), dma((4, 2)), dma((4, 2)), dma((4, 2)), dma((7,)), dma((7,)),
            dma((3, 8)), dma((3, 8)), dma((7,)), dma((7,)), dma((2,)), dma((4,)), dma((6,)), dma((2,)), dma((2,)),
        ],
        compiler_params=pltpu.CompilerParams(
            collective_id=0, has_side_effects=True, vmem_limit_bytes=58 * 2**20
        ),
        name="step",
    )(alignment, w_factors.T, query_weight, w_keyval, w_gate, output_weight, w_pair_out)


def place_kernel(update_ref, pair_ref, update_out, pair_out, rows, turned, pieces, *sems):
    row_sems, piece_sems, turned_sems, placed_sem = sems
    x = lax.axis_index("x_hi") * 2 + lax.axis_index("x_lo")
    y, z, core = lax.axis_index("y"), lax.axis_index("z"), lax.axis_index("core")
    row_loads = [
        pltpu.make_async_copy(update_ref.at[n], rows.at[n], row_sems.at[n]) for n in range(4)
    ]
    piece_loads = [
        pltpu.make_async_copy(pair_ref.at[n], pieces.at[n], piece_sems.at[n]) for n in range(8)
    ]
    for load in row_loads + piece_loads:
        load.start()
    copies = []

    def put(piece):
        there_core = flipped(core, piece % 2)
        away = piece // 2
        for step in range(4):
            there_y = lax.rem(y + there_core * away + (1 - there_core) * step, 4)
            there_z = lax.rem(z + there_core * step + (1 - there_core) * away, 4)
            for dx in range(4):
                there_x = lax.rem(x + dx, 4)
                copy = pltpu.make_async_copy(
                    pieces.at[piece, :, step * 4 + dx],
                    pair_out.at[
                        :, lax.rem(there_x, 2), there_y, there_z, there_x // 2, there_core
                    ],
                    placed_sem,
                )
                copy.start()
                copies.append(copy)

    for n in range(4):
        row_loads[n].wait()
        turned[n] = jnp.swapaxes(rows[n].astype(F32), 0, 1).astype(BF16)
        first = pl.multiple_of(seq_of(n) * 8, 8)
        copy = pltpu.make_async_copy(
            turned.at[n], update_out.at[:, pl.ds(first, 8), :], turned_sems.at[n]
        )
        copy.start()
        copies.append(copy)
        for piece in (2 * n, 2 * n + 1):
            piece_loads[piece].wait()
            put(piece)
    for copy in copies:
        copy.wait()


def place_call(update, pieces):
    dma = pltpu.SemaphoreType.DMA
    update, pair = pl.pallas_call(
        place_kernel,
        in_specs=[ANY_SPEC] * 2,
        out_specs=[ANY_SPEC] * 2,
        out_shape=[
            jax.ShapeDtypeStruct((96, 32, 256), BF16),
            jax.ShapeDtypeStruct((8, 2, 4, 4, 2, 2, 8, 128), BF16),
        ],
        scratch_shapes=[
            pltpu.VMEM((4, 8, 96, 256), BF16),
            pltpu.VMEM((4, 96, 8, 256), BF16),
            pltpu.VMEM((8, 8, 16, 8, 128), BF16),
            dma((4,)), dma((8,)), dma((4,)), dma,
        ],
        compiler_params=pltpu.CompilerParams(vmem_limit_bytes=58 * 2**20),
        name="place",
    )(update, pieces.reshape(8, 8, 16, 8, 128))
    return update, pair.reshape(8, 1024, 128)


def per_device(alignment, query_weight, w_keyval, w_gate, output_weight, w_factors, w_pair_out):
    update, pieces = step_call(
        alignment, w_factors, query_weight, w_keyval, w_gate, output_weight, w_pair_out
    )
    return place_call(update, pieces)


def solution(mesh):
    split = Mesh(mesh.devices.reshape(SIZES), AXES)
    in_specs = (P(SEQ, RES, None), P(), P(), P(), P(), P(), P())
    out_specs = (P(SEQ, RES, None), P(AXES, None, None))
    return jax.shard_map(
        per_device, mesh=split, in_specs=in_specs, out_specs=out_specs, check_vma=False
    )
```
